256 devices in a mesh: groups: 2 (over y), rows: 16 (over z), cols: 8 (over x, core).
Axes of the slice: x: 4, y: 2, z: 16, core: 2. Of those that a mesh axis runs over, the one named last changes fastest.
The devices are a block of a 4x16x16 slice.
Arguments:
- tokens: bfloat16 [448, 224, 256], P(('groups', 'rows'), 'cols'), parts along dimension 0, may hold values from -6 to 6
- cotangent: bfloat16 [224, 112, 512], P(('groups', 'rows'), 'cols'), parts along dimension 0, may hold values from -6 to 6
- shift_offsets: int32 [4], replicated, may hold values from 1 to 6
- norm2_gain: float32 [256], replicated, may hold values from 0.1 to 1.9
- qkv2: bfloat16 [256, 768], replicated, may hold values from -0.375 to 0.375
- proj2: bfloat16 [256, 256], replicated, may hold values from -0.375 to 0.375
- merge_gain: float32 [1024], replicated, may hold values from 0.1 to 1.9
- merge_weight: bfloat16 [1024, 512], replicated, may hold values from -0.1875 to 0.1875
- norm3_gain: float32 [512], replicated, may hold values from 0.1 to 1.9
- qkv3: bfloat16 [512, 1536], replicated, may hold values from -0.25 to 0.25
- proj3: bfloat16 [512, 512], replicated, may hold values from -0.25 to 0.25
Outputs:
- merged_out: bfloat16 [224, 112, 512], P(('groups', 'rows'), 'cols'), parts along dimension 0
- tokens_grad: bfloat16 [448, 224, 256], P(('groups', 'rows'), 'cols'), parts along dimension 0
- gain_grads: float32 [3584], P('groups'), parts along dimension 0
- qkv2_grad: bfloat16 [393216], P(('groups', 'rows', 'cols')), parts along dimension 0
- proj2_grad: bfloat16 [131072], P(('groups', 'rows', 'cols')), parts along dimension 0
- merge_grad: bfloat16 [1048576], P(('groups', 'rows', 'cols')), parts along dimension 0
- qkv3_grad: bfloat16 [1572864], P(('groups', 'rows', 'cols')), parts along dimension 0
- proj3_grad: bfloat16 [524288], P(('groups', 'rows', 'cols')), parts along dimension 0
The draws below stay inside these ranges and needn't reach their ends.
There are 2 independent parts, one for each index of `groups`. The reference program is written for one: setup_inputs(seed, part) draws one part's arguments, and reference() takes and returns one part's arrays. A program takes and returns all parts, laid end to end along the dimension named above; an argument that names none is the same for every part. Nothing has to cross between parts.
All inputs are finite; a program needn't handle non-finite values.
Results may differ from the reference program's by a relative error of at most 0.033.
Values may be sent and summed in bfloat16 or wider, within the bound.
No kernel may reach another device: no remote copies, remote signals or barrier semaphores. Data moves between devices by JAX's collectives and lax.ppermute only.
A program may use at most 128 MiB of HBM per device.

```python
import jax
import jax.numpy as jnp
from jax import lax

C2 = 256
C3 = 512
HEADS2 = 8
HEADS3 = 16
WIN = 7
H2 = 224
W2 = 224


def plant(array, key, smallest, top_value):
    extent = array.shape
    place = [jax.random.randint(jax.random.fold_in(key, axis), (), 0, extent[axis]) for axis in range(len(extent))]
    array = array.at[tuple(place)].set(smallest)
    longest = extent.index(max(extent))
    place[longest] = (place[longest] + 1) % extent[longest]
    return array.at[tuple(place)].set(top_value)


def shard_levels(own_key, shape, split, least, top_value):
    level = 1.0
    for dim, parts in split:
        heights = jax.random.uniform(jax.random.fold_in(jax.random.fold_in(own_key, 6), dim), (parts,), jnp.float32, least / len(split), top_value / len(split))
        level = level * jnp.repeat(jnp.exp(heights), shape[dim] // parts).reshape((-1,) + (1,) * (len(shape) - 1 - dim))
    return level


def noise(rng, extent, scale, bound, pieces=(), kind=jnp.bfloat16):
    result = jax.random.normal(rng, extent, jnp.float32) * scale
    if len(pieces) > 0:
        result = shard_levels(rng, extent, pieces, -0.22, 0.18) * result
    return jnp.clip(result, min=-bound, max=bound).astype(kind)


def setup_inputs(seed: int = 0, part: int = 0) -> dict:
    splits = jax.random.split(jax.random.key(seed), 12)
    part_splits = jax.random.split(jax.random.fold_in(splits[11], part), 12)
    return {
        "tokens": noise(part_splits[0], (H2, W2, C2), 1.0, 6.0, ((0, 16), (1, 8))),
        "cotangent": noise(part_splits[1], (H2 // 2, W2 // 2, C3), 1.0, 6.0, ((0, 16), (1, 8))),
        "shift_offsets": plant(jax.random.randint(splits[2], (4,), 1, WIN), jax.random.fold_in(splits[2], 1), 1, WIN - 1).astype(jnp.int32),
        "norm2_gain": jnp.clip(1.0 + 0.18 * jax.random.normal(splits[3], (C2,), jnp.float32), 0.1, 1.9),
        "qkv2": noise(splits[4], (C2, 3 * C2), C2 ** -0.5, 0.375),
        "proj2": noise(splits[5], (C2, C2), C2 ** -0.5, 0.375),
        "merge_gain": jnp.clip(1.0 + 0.18 * jax.random.normal(splits[6], (4 * C2,), jnp.float32), 0.1, 1.9),
        "merge_weight": noise(splits[7], (4 * C2, C3), (4 * C2) ** -0.5, 0.1875),
        "norm3_gain": jnp.clip(1.0 + 0.18 * jax.random.normal(splits[8], (C3,), jnp.float32), 0.1, 1.9),
        "qkv3": noise(splits[9], (C3, 3 * C3), C3 ** -0.5, 0.25),
        "proj3": noise(splits[10], (C3, C3), C3 ** -0.5, 0.25),
    }


EPSILON = 1e-05
MASKED = -100.0

def normalize(inputs, gain):
    widened = inputs.astype(jnp.float32)
    centred = widened - lax.optimization_barrier(jnp.mean(widened, axis=-1, keepdims=True))
    spread = lax.optimization_barrier(jnp.mean(centred * centred, axis=-1, keepdims=True))
    return (centred * lax.rsqrt(spread + EPSILON) * gain).astype(jnp.bfloat16)

def attend(packed, heads, region):
    count, window_area, triple = packed.shape
    width = triple // 3
    head_size = width // heads
    queries = packed[:, :, :width].astype(jnp.float32).reshape(count, window_area, heads, head_size)
    key_part = packed[:, :, width:2 * width].astype(jnp.float32).reshape(count, window_area, heads, head_size)
    values = packed[:, :, 2 * width:].astype(jnp.float32).reshape(count, window_area, heads, head_size)
    scores = jnp.einsum('nphd,nqhd->nhpq', queries, key_part) * head_size ** (-0.5)
    scores = scores + region[:, None, :, :]
    raised = jnp.exp(scores)
    weights = (raised / lax.optimization_barrier(jnp.sum(raised, axis=-1, keepdims=True))).astype(jnp.bfloat16)
    mixed = jnp.einsum('nhpq,nqhd->nphd', weights.astype(jnp.float32), values)
    return mixed.reshape(count, window_area, width).astype(jnp.bfloat16)

def to_windows(values, window):
    height, breadth, width = values.shape
    shaped = values.reshape(height // window, window, breadth // window, window, width)
    return shaped.transpose(0, 2, 1, 3, 4).reshape(-1, window * window, width)

def from_windows(windows, height, breadth, window):
    width = windows.shape[-1]
    shaped = windows.reshape(height // window, breadth // window, window, window, width)
    return shaped.transpose(0, 2, 1, 3, 4).reshape(height, breadth, width)

def pair_join(values):
    height, breadth, width = values.shape
    shaped = values.reshape(height // 2, 2, breadth // 2, 2, width)
    return shaped.transpose(0, 2, 3, 1, 4).reshape(height // 2, breadth // 2, 4 * width)

def cyclic(values, start, axis):
    doubled = jnp.concatenate([values, values], axis=axis)
    return lax.dynamic_slice_in_dim(doubled, start.astype(jnp.int32), values.shape[axis], axis)

def region_bias(row_coords, col_coords, height, breadth, shift_rows, shift_cols):
    row_label = jnp.where(row_coords < height - WIN, 0, jnp.where(row_coords < height - shift_rows, 1, 2))
    col_label = jnp.where(col_coords < breadth - WIN, 0, jnp.where(col_coords < breadth - shift_cols, 1, 2))
    labels = (row_label[:, None] * 3 + col_label[None, :]).astype(jnp.int32)
    windowed = to_windows(labels[:, :, None], WIN)[:, :, 0]
    return jnp.where(windowed[:, :, None] == windowed[:, None, :], 0.0, MASKED).astype(jnp.float32)

def shifted_block(inputs, normed, shift_rows, shift_cols, qkv, proj, heads):
    height, breadth, width = inputs.shape
    rolled = to_windows(cyclic(cyclic(normed, shift_rows, 0), shift_cols, 1), WIN)
    bias = region_bias(jnp.arange(height, dtype=jnp.int32), jnp.arange(breadth, dtype=jnp.int32), height, breadth, shift_rows, shift_cols)
    packed = jnp.dot(rolled.reshape(-1, width), qkv, preferred_element_type=jnp.float32)
    packed = packed.astype(jnp.bfloat16).reshape(rolled.shape[0], WIN * WIN, 3 * width)
    mixed = attend(packed, heads, bias)
    projected = jnp.dot(mixed.reshape(-1, width), proj, preferred_element_type=jnp.float32).astype(jnp.bfloat16)
    grid = from_windows(projected.reshape(-1, WIN * WIN, width), height, breadth, WIN)
    restored = cyclic(cyclic(grid, height - shift_rows, 0), breadth - shift_cols, 1)
    return (inputs.astype(jnp.float32) + restored.astype(jnp.float32)).astype(jnp.bfloat16)

def forward(tokens, norm2_gain, qkv2, proj2, merge_gain, merge_weight, norm3_gain, qkv3, proj3, shift_offsets):
    height, breadth, narrow = tokens.shape
    wide_width = qkv3.shape[0]
    normed = normalize(tokens, norm2_gain)
    section_two = shifted_block(tokens, normed, shift_offsets[0], shift_offsets[1], qkv2, proj2, HEADS2)
    merged_norm = normalize(pair_join(section_two), merge_gain)
    merged = jnp.dot(merged_norm.reshape(-1, 4 * narrow), merge_weight, preferred_element_type=jnp.float32)
    merged = merged.astype(jnp.bfloat16).reshape(height // 2, breadth // 2, wide_width)
    normed_three = normalize(merged, norm3_gain)
    return shifted_block(merged, normed_three, shift_offsets[2], shift_offsets[3], qkv3, proj3, HEADS3)

def reference(tokens, cotangent, shift_offsets, norm2_gain, qkv2, proj2, merge_gain, merge_weight, norm3_gain, qkv3, proj3):

    def run(tok, gain_two, weight_qkv2, weight_proj2, gain_merge, weight_merge, gain_three, weight_qkv3, weight_proj3):
        return forward(tok, gain_two, weight_qkv2, weight_proj2, gain_merge, weight_merge, gain_three, weight_qkv3, weight_proj3, shift_offsets)
    outcome, pullback = jax.vjp(run, tokens, norm2_gain, qkv2, proj2, merge_gain, merge_weight, norm3_gain, qkv3, proj3)
    grads = pullback(cotangent)
    gains = jnp.concatenate([grads[1], grads[4], grads[6]])
    return (outcome, grads[0], gains, grads[2].reshape(-1), grads[3].reshape(-1), grads[5].reshape(-1), grads[7].reshape(-1), grads[8].reshape(-1))
```

```python
import jax
import jax.numpy as jnp
from jax import lax
from jax.experimental import pallas as pl
from jax.experimental.pallas import tpu as pltpu
from jax.sharding import Mesh
from jax.sharding import PartitionSpec as P

HEADS2 = 8
HEADS3 = 16
WIN = 7
AREA = WIN * WIN
SLOT = 64
PAIR = 2 * SLOT
TILE = 128
HEAD = 32
EDGE = WIN - 1
COLS = ("cols_0", "cols_1")
ROWS_COLS = ("rows", "cols_0", "cols_1")
GROUPS_ROWS_COLS = ("groups", "rows", "cols_0", "cols_1")

EPSILON = 1e-05
MASKED = -100.0
APART = -1e30
BF = jnp.bfloat16
F32 = jnp.float32


def up16(count):
    return -(-count // 16) * 16


def mm(a, b):
    return lax.dot_general(a, b, (((1,), (0,)), ((), ())), preferred_element_type=F32)


def mm_nt(a, b):
    return lax.dot_general(a, b, (((1,), (1,)), ((), ())), preferred_element_type=F32)


def mm_tn(a, b):
    return lax.dot_general(a, b, (((0,), (0,)), ((), ())), preferred_element_type=F32)


def pick(selection, source):
    return mm(selection, source).astype(BF)


def norm_parts(values):
    centred = values - jnp.mean(values, axis=-1, keepdims=True)
    spread = jnp.mean(centred * centred, axis=-1, keepdims=True)
    scale = lax.rsqrt(spread + EPSILON)
    return centred * scale, scale


def normed(values, gain):
    return (norm_parts(values)[0] * gain).astype(BF)


def norm_back(values, gain, upstream):
    unit, scale = norm_parts(values)
    inner = upstream * gain
    along = jnp.mean(inner * unit, axis=-1, keepdims=True)
    grad = scale * (inner - jnp.mean(inner, axis=-1, keepdims=True) - unit * along)
    return grad.astype(BF), jnp.sum(upstream * unit, axis=0, keepdims=True)


def lane_head(shape):
    return lax.broadcasted_iota(jnp.int32, shape, 1) // HEAD


def stacked(block):
    heads = lane_head((1, TILE))
    parts = [block * (heads == h).astype(F32).astype(BF) for h in range(TILE // HEAD)]
    return jnp.concatenate(parts, axis=0)


def unstacked(tall):
    heads = lane_head((PAIR, TILE))
    out = tall[:PAIR]
    for h in range(1, TILE // HEAD):
        out = jnp.where(heads == h, tall[h * PAIR : (h + 1) * PAIR], out)
    return out


def soft(queries, keys, bias):
    tall = stacked(queries)
    raised = jnp.exp(mm_nt(tall, keys) * HEAD ** (-0.5) + bias)
    return tall, raised / jnp.sum(raised, axis=-1, keepdims=True)


def tiled_bias(bias):
    return jnp.concatenate([bias] * (TILE // HEAD), axis=0)


def attend_forward(packed, width, bias_of, store):
    for g in range(packed.shape[0] // PAIR):
        rows = slice(g * PAIR, (g + 1) * PAIR)
        bias = tiled_bias(bias_of(g))
        for t in range(width // TILE):
            q, k, v = (packed[rows, p * width + t * TILE :][:, :TILE] for p in range(3))
            share = soft(q, k, bias)[1].astype(BF)
            store(rows, slice(t * TILE, (t + 1) * TILE), unstacked(mm(share, v)).astype(BF))


def attend_backward(packed, upstream, width, bias_of, store):
    for g in range(packed.shape[0] // PAIR):
        rows = slice(g * PAIR, (g + 1) * PAIR)
        bias = tiled_bias(bias_of(g))
        for t in range(width // TILE):
            q, k, v = (packed[rows, p * width + t * TILE :][:, :TILE] for p in range(3))
            tall, share = soft(q, k, bias)
            above = stacked(upstream[rows, t * TILE : (t + 1) * TILE])
            d_share = mm_nt(above, v).astype(BF).astype(F32)
            along = jnp.sum(d_share * share, axis=-1, keepdims=True)
            d_scores = (share * (d_share - along) * HEAD ** (-0.5)).astype(BF)
            grads = (
                unstacked(mm(d_scores, k)),
                mm_tn(d_scores, tall),
                mm_tn(share.astype(BF), above),
            )
            for p, grad in enumerate(grads):
                at = p * width + t * TILE
                store(rows, slice(at, at + TILE), grad.astype(BF))


def put_pieces(grad, out, block, lanes, halves=1):
    cores, xs = out.shape[:2]
    size = grad.shape[0] // (cores * xs * halves)
    width = grad.shape[1]
    for h in range(halves):
        for c in range(cores):
            for x in range(xs):
                at = ((h * cores + c) * xs + x) * size
                lo = lanes + h * width
                out[c, x, block * size : (block + 1) * size, lo : lo + width] = grad[
                    at : at + size
                ].astype(BF)


def weight_grad(acts, order, upstream, out, lanes, halves=1):
    side = order.shape[0]
    for block in range(acts.shape[1] // side):
        moved = pick_cols(acts[:, block * side : (block + 1) * side], order)
        put_pieces(mm_tn(moved, upstream), out, block, lanes, halves)


def pick_cols(acts, order):
    return mm(acts, order).astype(BF)


def put_edges(values, edges, outs):
    sent = pick(edges, values)
    at = 0
    for out in outs:
        out[...] = sent[at : at + out.shape[0]]
        at += out.shape[0]


def joined(refs):
    return jnp.concatenate([r[...] for r in refs], axis=0)


def two_forward(
    t0, t1, t2, t3, gain, qkv, proj, sel, bias, edges, rolled_o, packed_o, mixed_o, wins_o, e0, e1, e2
):
    tokens = pick(sel[...], joined((t0, t1, t2, t3)))
    rolled = normed(tokens.astype(F32), gain[...])
    rolled_o[...] = rolled
    packed_o[...] = mm(rolled, qkv[...]).astype(BF)

    def store(rows, lanes, value):
        mixed_o[rows, lanes] = value

    attend_forward(packed_o, rolled.shape[1], lambda g: bias[g], store)
    projected = mm(mixed_o[...], proj[...]).astype(BF)
    wins_o[...] = projected
    put_edges(projected, edges[...], (e0, e1, e2))


def merge_forward(
    tokens, w0, w1, w2, w3, sel_tokens, sel_back, gain, weight, gain3, edges,
    two_o, tokens_o, norm_o, merged_o, normed_o, e0, e1, e2,
):
    laid = pick(sel_tokens[...], tokens[...])
    back = pick(sel_back[...], joined((w0, w1, w2, w3)))
    two = (laid.astype(F32) + back.astype(F32)).astype(BF)
    tokens_o[...] = laid
    size = two.shape[0] // 4
    wide = jnp.concatenate([two[k * size : (k + 1) * size] for k in range(4)], axis=1)
    two_o[...] = wide
    merged_norm = normed(wide.astype(F32), gain[...])
    norm_o[...] = merged_norm
    merged = mm(merged_norm, weight[...]).astype(BF)
    merged_o[...] = merged
    three = normed(merged.astype(F32), gain3[...])
    normed_o[...] = three
    put_edges(three, edges[...], (e0, e1, e2))


def three_both(
    n0, n1, n2, n3, c0, c1, c2, c3, qkv, proj, sel, bias, edges, order,
    both_o, grad_o, e0, e1, e2, packed, mixed, d_packed,
):
    rolled = pick(sel[...], joined((n0, n1, n2, n3)))
    above = pick(sel[...], joined((c0, c1, c2, c3)))
    width = rolled.shape[1]
    packed[...] = mm(rolled, qkv[...]).astype(BF)

    def store_mixed(rows, lanes, value):
        mixed[rows, lanes] = value

    def store_grad(rows, lanes, value):
        d_packed[rows, lanes] = value

    attend_forward(packed, width, lambda g: bias[...], store_mixed)
    projected = mm(mixed[...], proj[...]).astype(BF)
    d_mixed = mm_nt(above, proj[...]).astype(BF)
    attend_backward(packed, d_mixed, width, lambda g: bias[...], store_grad)
    d_rolled = mm_nt(d_packed[...], qkv[...]).astype(BF)
    both = jnp.concatenate([projected, d_rolled], axis=1)
    both_o[...] = both
    put_edges(both, edges[...], (e0, e1, e2))
    weight_grad(rolled, order[...], d_packed[...], grad_o, 0)
    weight_grad(mixed[...], order[...], above, grad_o, 3 * width)


def merge_backward(
    b0, b1, b2, b3, merged, cot, two, norm, sel_back, gain3, gain, weight, edges, order,
    out_o, d_two_o, grad_o, gm_o, g3_o, e0, e1, e2,
):
    back = pick(sel_back[...], joined((b0, b1, b2, b3)))
    width = merged.shape[1]
    base = merged[...].astype(F32)
    out = base + back[:, :width].astype(F32)
    rows, cols = out_o.shape[:2]
    pad = out.shape[0] // rows
    for r in range(rows):
        out_o[r] = out[r * pad : r * pad + cols].astype(BF)
    d_normed = back[:, width:].astype(F32)
    d_merged, g3 = norm_back(base, gain3[...], d_normed)
    g3_o[...] = g3
    d_rows = (cot[...].astype(F32) + d_merged.astype(F32)).astype(BF)
    d_norm = mm_nt(d_rows, weight[...]).astype(BF).astype(F32)
    d_wide, gm = norm_back(two[...].astype(F32), gain[...], d_norm)
    gm_o[...] = gm
    quarter = d_wide.shape[1] // 4
    d_two = jnp.concatenate([d_wide[:, k * quarter : (k + 1) * quarter] for k in range(4)], axis=0)
    d_two_o[...] = d_two
    put_edges(d_two, edges[...], (e0, e1, e2))
    weight_grad(norm[...], order[...], d_rows, grad_o, 0, halves=2)


def two_backward(
    d0, d1, d2, d3, mixed, packed, rolled, qkv, proj, gain, sel, bias, edges, order, gm, g3,
    wins_o, grad_o, e0, e1, e2, d_packed,
):
    above = pick(sel[...], joined((d0, d1, d2, d3)))
    width = above.shape[1]
    d_mixed = mm_nt(above, proj[...]).astype(BF)

    def store_grad(rows, lanes, value):
        d_packed[rows, lanes] = value

    attend_backward(packed, d_mixed, width, lambda g: bias[g], store_grad)
    d_rolled = mm_nt(d_packed[...], qkv[...]).astype(BF)
    wins_o[...] = d_rolled
    put_edges(d_rolled, edges[...], (e0, e1, e2))
    weight_grad(rolled[...], order[...], d_packed[...], grad_o, 0)
    weight_grad(mixed[...], order[...], above, grad_o, 3 * width)
    g2 = jnp.sum(d_rolled.astype(F32) * rolled[...].astype(F32), axis=0, keepdims=True) / gain[...]
    blank = jnp.zeros((1, width), F32)
    second = jnp.concatenate([g3[...], g2, blank], axis=1)
    line = lax.broadcasted_iota(jnp.int32, (16, 4 * width), 0)
    gains = jnp.where(line == 0, gm[...], jnp.where(line == 1, second, 0.0)).astype(BF)
    cores, xs, rows = grad_o.shape[:3]
    for c in range(cores):
        for x in range(xs):
            grad_o[c, x, rows - 16 :, :] = gains


def tokens_backward(w0, w1, w2, w3, tokens, d_two, gain, sel_back, sel_out, out_o):
    d_normed = pick(sel_back[...], joined((w0, w1, w2, w3)))
    d_norm, _ = norm_back(tokens[...].astype(F32), gain[...], d_normed.astype(F32))
    total = (d_two[...].astype(F32) + d_norm.astype(F32)).astype(BF)
    laid = pick(sel_out[...], total)
    rows, cols = out_o.shape[:2]
    pad = laid.shape[0] // rows
    for r in range(rows):
        out_o[r] = laid[r * pad : r * pad + cols]


def call(body, outs, args, name, flops, scratch=()):
    return pl.pallas_call(
        body,
        out_shape=[jax.ShapeDtypeStruct(shape, kind) for shape, kind in outs],
        scratch_shapes=[pltpu.VMEM(shape, kind) for shape, kind in scratch],
        cost_estimate=pl.CostEstimate(flops=flops, transcendentals=0, bytes_accessed=4 << 20),
        compiler_params=pltpu.CompilerParams(vmem_limit_bytes=48 << 20),
        name=name,
    )(*args)


def selection(wanted, width):
    return (wanted[:, None] == jnp.arange(width, dtype=jnp.int32)[None, :]).astype(BF)


def window_rows(count, per_line):
    p = jnp.arange(count * SLOT, dtype=jnp.int32)
    w, t = p // SLOT, p % SLOT
    row = (w // per_line) * WIN + t // WIN
    col = (w % per_line) * WIN + t % WIN
    return t < AREA, row, col


def window_place(row, col, per_line):
    return ((row // WIN) * per_line + col // WIN) * SLOT + (row % WIN) * WIN + col % WIN


def by_side(low, right, main, rows, cols, corner):
    return jnp.where(low, jnp.where(right, corner, rows), jnp.where(right, cols, main))


def bias_blocks(valid, row, col, tall, broad, shift_rows, shift_cols, row0, col0):
    def label(at, extent, shift):
        return jnp.where(at < extent - WIN, 0, jnp.where(at < extent - shift, 1, 2))

    marks = label(row + row0, tall, shift_rows) * 3 + label(col + col0, broad, shift_cols)
    marks = jnp.where(valid, marks, -1).reshape(-1, PAIR)
    window = (jnp.arange(PAIR, dtype=jnp.int32) // SLOT)[None, :]
    good = marks >= 0
    near = (window[:, :, None] == window[:, None, :]) & (good[:, :, None] == good[:, None, :])
    same = marks[:, :, None] == marks[:, None, :]
    return jnp.where(near, jnp.where(same, 0.0, MASKED), APART).astype(F32)


def chunk_order(depth, ranks, halves):
    rows, xs, cores = ranks
    side = 256
    per_row = depth // rows
    near = side // per_row
    sub = depth // (rows * xs * cores)
    part = sub // halves
    at = jnp.arange(side, dtype=jnp.int32)
    s = at % part
    r = (at // part) % near
    x = (at // (part * near) + lax.axis_index("cols_0")) % xs
    c = (at // (part * near * xs) + 1 + lax.axis_index("cols_1")) % cores
    h = at // (part * near * xs * cores)
    source = r * per_row + (x * cores + c) * sub + h * part + s
    return (jnp.arange(side, dtype=jnp.int32)[:, None] == source[None, :]).astype(BF)


def moved(value, axis, by):
    count = lax.axis_size(axis)
    return lax.ppermute(value, axis, [(i, (i + by) % count) for i in range(count)])


def moved_across(value, by):
    rows, cols = lax.axis_size("rows"), lax.axis_size(COLS)
    pairs = [
        (i * cols + j, ((i + by) % rows) * cols + (j + by) % cols)
        for i in range(rows)
        for j in range(cols)
    ]
    return lax.ppermute(value, ROWS_COLS, pairs)


def to_neighbours(pieces, by):
    rows, cols, corner = pieces
    return moved_across(corner, by), moved(rows, "rows", by), moved(cols, COLS, by)


def exchanged(pieces, by):
    corner, rows, cols = to_neighbours(pieces, by)
    return rows, cols, corner


def sum_core(grads):
    got = moved(grads[0], "cols_1", 1)
    return (grads[1].astype(F32) + got.astype(F32)).astype(BF)


def sum_line(grads):
    count = lax.axis_size("cols_0")
    held = [grads[0]] + [moved(grads[j], "cols_0", j) for j in range(1, count)]
    held = [h.astype(F32) for h in held]
    while len(held) > 1:
        half = len(held) // 2
        held = [held[j] + held[j + half] for j in range(half)]
    return held[0].astype(BF)


def sum_rows(blocks):
    spread = lax.all_to_all(blocks, "rows", 0, 0)
    return jnp.sum(spread.astype(F32), axis=0)


def on_device(
    tokens,
    cotangent,
    shift_offsets,
    norm2_gain,
    qkv2,
    proj2,
    merge_gain,
    merge_weight,
    norm3_gain,
    qkv3,
    proj3,
):
    tile_rows, tile_cols, narrow = tokens.shape
    wide = qkv3.shape[0]
    ranks = tuple(lax.axis_size(a) for a in ROWS_COLS)
    row_rank, col_rank = lax.axis_index("rows"), lax.axis_index(COLS)
    tall, broad = tile_rows * ranks[0], tile_cols * ranks[1] * ranks[2]
    three_rows, three_cols = tile_rows // 2, tile_cols // 2
    s0, s1, s2, s3 = (shift_offsets[i] for i in range(4))
    i32 = jnp.int32

    pad = up16(tile_cols)
    tokens_p = jnp.pad(tokens, ((0, 0), (0, pad - tile_cols), (0, 0))).reshape(-1, narrow)
    token_pieces = exchanged(
        (
            tokens_p[: EDGE * pad],
            tokens[:, :8].reshape(-1, narrow),
            tokens[:EDGE, :8].reshape(-1, narrow),
        ),
        -1,
    )
    pad3 = up16(three_cols)
    cot_p = jnp.pad(cotangent, ((0, 0), (0, pad3 - three_cols), (0, 0))).reshape(-1, wide)

    def flat_pad(piece):
        flat = piece.reshape(-1, piece.shape[-1])
        return jnp.pad(flat, ((0, up16(flat.shape[0]) - flat.shape[0]), (0, 0)))

    cot_pieces = exchanged(
        (
            cot_p[: EDGE * pad3],
            flat_pad(cotangent[:, :EDGE]),
            flat_pad(cotangent[:EDGE, :EDGE]),
        ),
        -1,
    )

    line2 = tile_cols // WIN
    count2 = line2 * (tile_rows // WIN)
    valid, row, col = window_rows(count2, line2)
    bias2 = bias_blocks(
        valid, row, col, tall, broad, s0, s1, row_rank * tile_rows, col_rank * tile_cols
    )
    far_row, far_col = row + s0, col + s1
    low, right = far_row >= tile_rows, far_col >= tile_cols
    a, b = far_row - tile_rows, far_col - tile_cols
    main_n = tile_rows * pad
    rows_n, cols_n = EDGE * pad, tile_rows * 8
    place = by_side(
        low,
        right,
        far_row * pad + far_col,
        main_n + a * pad + far_col,
        main_n + rows_n + far_row * 8 + b,
        main_n + rows_n + cols_n + a * 8 + b,
    )
    sel_a = selection(jnp.where(valid, place, -1), main_n + rows_n + cols_n + EDGE * 8)

    er, ec, ex = up16(EDGE * tile_cols), up16(tile_rows * EDGE), up16(EDGE * EDGE)

    def edge_places(at_row, at_col, rows, cols, first_row, first_col):
        def strip(height, breadth, r0, c0):
            p = jnp.arange(up16(height * breadth), dtype=i32)
            r, c = p // breadth + r0, p % breadth + c0
            return jnp.where(p < height * breadth, at(r, c), -1)

        def at(r, c):
            return at_row(r, c) if at_col is None else at_col(r, c)

        return jnp.concatenate(
            [
                strip(EDGE, cols, first_row, 0),
                strip(rows, EDGE, 0, first_col),
                strip(EDGE, EDGE, first_row, first_col),
            ]
        )

    def in_windows2(r, c):
        return window_place(r, c, line2)

    size3 = three_rows * pad3

    def in_planes(r, c):
        return ((c % 2) * 2 + r % 2) * size3 + (r // 2) * pad3 + c // 2

    tail_edges2 = selection(
        edge_places(in_windows2, None, tile_rows, tile_cols, tile_rows - EDGE, tile_cols - EDGE),
        count2 * SLOT,
    )
    head_edges2 = selection(
        edge_places(in_planes, None, tile_rows, tile_cols, 0, 0), 4 * size3
    )
    q = jnp.arange(4 * size3, dtype=i32)
    k, m = q // size3, q % size3
    real = m % pad3 < three_cols
    grid_row, grid_col = 2 * (m // pad3) + k % 2, 2 * (m % pad3) + k // 2
    sel_tokens = selection(jnp.where(real, grid_row * pad + grid_col, -1), main_n)
    g = jnp.arange(main_n, dtype=i32)
    sel_out = selection(
        jnp.where(g % pad < tile_cols, in_planes(g // pad, g % pad), -1), 4 * size3
    )
    near_row, near_col = grid_row - s0, grid_col - s1
    up, left = near_row < 0, near_col < 0
    n2 = count2 * SLOT
    place = by_side(
        up,
        left,
        in_windows2(near_row, near_col),
        n2 + (near_row + EDGE) * tile_cols + near_col,
        n2 + er + near_row * EDGE + near_col + EDGE,
        n2 + er + ec + (near_row + EDGE) * EDGE + near_col + EDGE,
    )
    sel_b = selection(jnp.where(real, place, -1), n2 + er + ec + ex)
    n4 = 4 * size3
    place = by_side(
        low,
        right,
        in_planes(far_row, far_col),
        n4 + a * tile_cols + far_col,
        n4 + er + far_row * EDGE + b,
        n4 + er + ec + a * EDGE + b,
    )
    sel_e = selection(jnp.where(valid, place, -1), n4 + er + ec + ex)

    line3 = three_cols // WIN
    count3 = line3 * (three_rows // WIN)
    valid3, row3, col3 = window_rows(count3, line3)
    bias3 = bias_blocks(
        valid3,
        row3,
        col3,
        tall // 2,
        broad // 2,
        s2,
        s3,
        row_rank * three_rows,
        col_rank * three_cols,
    )[0]
    far_row, far_col = row3 + s2, col3 + s3
    low, right = far_row >= three_rows, far_col >= three_cols
    a, b = far_row - three_rows, far_col - three_cols
    hr, hc, hx = EDGE * pad3, up16(three_rows * EDGE), up16(EDGE * EDGE)
    place = by_side(
        low,
        right,
        far_row * pad3 + far_col,
        size3 + a * pad3 + far_col,
        size3 + hr + far_row * EDGE + b,
        size3 + hr + hc + a * EDGE + b,
    )
    sel3 = selection(jnp.where(valid3, place, -1), size3 + hr + hc + hx)

    def strip3(height, breadth, stride):
        p = jnp.arange(up16(height * breadth), dtype=i32)
        return jnp.where(p < height * breadth, (p // breadth) * stride + p % breadth, -1)

    head_edges3 = selection(
        jnp.concatenate(
            [
                jnp.arange(hr, dtype=i32),
                strip3(three_rows, EDGE, pad3),
                strip3(EDGE, EDGE, pad3),
            ]
        ),
        size3,
    )

    def in_windows3(r, c):
        return window_place(r, c, line3)

    tail_edges3 = selection(
        edge_places(
            in_windows3, None, three_rows, three_cols, three_rows - EDGE, three_cols - EDGE
        ),
        count3 * SLOT,
    )
    tr = up16(EDGE * three_cols)
    m = jnp.arange(size3, dtype=i32)
    near_row, near_col = m // pad3 - s2, m % pad3 - s3
    n3 = count3 * SLOT
    place = by_side(
        near_row < 0,
        near_col < 0,
        in_windows3(near_row, near_col),
        n3 + (near_row + EDGE) * three_cols + near_col,
        n3 + tr + near_row * EDGE + near_col + EDGE,
        n3 + tr + hc + (near_row + EDGE) * EDGE + near_col + EDGE,
    )
    sel3b = selection(jnp.where(m % pad3 < three_cols, place, -1), n3 + tr + hc + hx)
    order2 = chunk_order(narrow, ranks, 1)
    order3 = chunk_order(wide, ranks, 1)
    order_m = chunk_order(4 * narrow, ranks, 2)
    gain2, gain_m, gain3 = norm2_gain[None], merge_gain[None], norm3_gain[None]

    rolled, packed, mixed, wins, e0, e1, e2 = call(
        two_forward,
        [
            ((n2, narrow), BF),
            ((n2, 3 * narrow), BF),
            ((n2, narrow), BF),
            ((n2, narrow), BF),
            ((er, narrow), BF),
            ((ec, narrow), BF),
            ((ex, narrow), BF),
        ],
        (tokens_p, *token_pieces, gain2, qkv2, proj2, sel_a, bias2, tail_edges2),
        "two_forward",
        1 << 30,
    )
    back = exchanged((e0, e1, e2), 1)
    two, tokens_q, merged_norm, merged, normed3, e0, e1, e2 = call(
        merge_forward,
        [
            ((size3, 4 * narrow), BF),
            ((n4, narrow), BF),
            ((size3, 4 * narrow), BF),
            ((size3, wide), BF),
            ((size3, wide), BF),
            ((hr, wide), BF),
            ((hc, wide), BF),
            ((hx, wide), BF),
        ],
        (
            tokens_p,
            wins,
            *back,
            sel_tokens,
            sel_b,
            gain_m,
            merge_weight,
            gain3,
            head_edges3,
        ),
        "merge_forward",
        1 << 30,
    )
    ahead = exchanged((e0, e1, e2), -1)
    xs, cores = ranks[1], ranks[2]
    both, grads_a, e0, e1, e2 = call(
        three_both,
        [
            ((n3, 2 * wide), BF),
            ((cores, xs, wide // (xs * cores), 4 * wide), BF),
            ((tr, 2 * wide), BF),
            ((hc, 2 * wide), BF),
            ((hx, 2 * wide), BF),
        ],
        (
            normed3,
            *ahead,
            cot_p,
            *cot_pieces,
            qkv3,
            proj3,
            sel3,
            bias3,
            tail_edges3,
            order3,
        ),
        "three_both",
        1 << 30,
        scratch=[((n3, 3 * wide), BF), ((n3, wide), BF), ((n3, 3 * wide), BF)],
    )
    back = exchanged((e0, e1, e2), 1)
    merged_out, d_two, grads_b, grad_m, grad_3, e0, e1, e2 = call(
        merge_backward,
        [
            ((three_rows, three_cols, wide), BF),
            ((n4, narrow), BF),
            ((cores, xs, wide // (xs * cores), 2 * wide), BF),
            ((1, 4 * narrow), F32),
            ((1, wide), F32),
            ((er, narrow), BF),
            ((ec, narrow), BF),
            ((ex, narrow), BF),
        ],
        (
            both,
            *back,
            merged,
            cot_p,
            two,
            merged_norm,
            sel3b,
            gain3,
            gain_m,
            merge_weight,
            head_edges2,
            order_m,
        ),
        "merge_backward",
        1 << 30,
    )
    ahead = exchanged((e0, e1, e2), -1)
    share2 = narrow // (xs * cores)
    wins, grads_c, e0, e1, e2 = call(
        two_backward,
        [
            ((n2, narrow), BF),
            ((cores, xs, share2 + 16, 4 * narrow), BF),
            ((er, narrow), BF),
            ((ec, narrow), BF),
            ((ex, narrow), BF),
        ],
        (
            d_two,
            *ahead,
            mixed,
            packed,
            rolled,
            qkv2,
            proj2,
            gain2,
            sel_e,
            bias2,
            tail_edges2,
            order2,
            grad_m,
            grad_3,
        ),
        "two_backward",
        1 << 30,
        scratch=[((n2, 3 * narrow), BF)],
    )
    back = exchanged((e0, e1, e2), 1)
    (tokens_grad,) = call(
        tokens_backward,
        [((tile_rows, tile_cols, narrow), BF)],
        (wins, *back, tokens_q, d_two, gain2, sel_b, sel_out),
        "tokens_backward",
        1 << 30,
    )

    line_a = sum_line(sum_core(grads_a))
    line_b = sum_line(sum_core(grads_b))
    line_c = sum_line(sum_core(grads_c))
    rows = ranks[0]
    early = jnp.concatenate([line_a, line_b], axis=1)
    early = sum_rows(early.reshape(rows, -1, early.shape[1]))
    gains = jnp.broadcast_to(line_c[share2 : share2 + 2][None], (rows, 2, 4 * narrow))
    late = line_c[:share2].reshape(rows, -1, 4 * narrow)
    late = sum_rows(jnp.concatenate([late, gains], axis=1))
    sub2 = late.shape[0] - 2
    gain_sums = jnp.concatenate(
        [late[sub2 + 1, wide : wide + narrow], late[sub2], late[sub2 + 1, :wide]]
    )
    chunk2 = late[:sub2].astype(BF)
    chunk3 = early.astype(BF)
    halves = [chunk3[:, (4 + h) * wide : (5 + h) * wide] for h in range(2)]
    return (
        merged_out,
        tokens_grad,
        gain_sums,
        chunk2[:, : 3 * narrow].reshape(-1),
        chunk2[:, 3 * narrow :].reshape(-1),
        jnp.concatenate(halves, axis=0).reshape(-1),
        chunk3[:, : 3 * wide].reshape(-1),
        chunk3[:, 3 * wide : 4 * wide].reshape(-1),
    )


def solution(mesh):
    cores = 2
    split = Mesh(
        mesh.devices.reshape(
            mesh.shape["groups"], mesh.shape["rows"], mesh.shape["cols"] // cores, cores
        ),
        ("groups", "rows", "cols_0", "cols_1"),
    )
    tiles = P(("groups", "rows"), COLS, None)
    flat = P(GROUPS_ROWS_COLS)
    return jax.shard_map(
        on_device,
        mesh=split,
        in_specs=(tiles, tiles) + (P(),) * 9,
        out_specs=(tiles, tiles, P("groups"), flat, flat, flat, flat, flat),
        check_vma=False,
    )
```

```python
import jax
import jax.numpy as jnp
from jax import lax
from jax.experimental import pallas as pl
from jax.experimental.pallas import tpu as pltpu
from jax.sharding import Mesh
from jax.sharding import PartitionSpec as P


WIN = 7
AREA = WIN * WIN
SLOT = 64
PAIR = 2 * SLOT
TILE = 128
HEAD = 32
EDGE = WIN - 1
COLS = ("cols_0", "cols_1")
ROWS_COLS = ("rows", "cols_0", "cols_1")
GROUPS_ROWS_COLS = ("groups", "rows", "cols_0", "cols_1")

EPSILON = 1e-05
MASKED = -100.0
APART = -1e30
BF = jnp.bfloat16
F32 = jnp.float32


def up16(count):
    return -(-count // 16) * 16


def mm(a, b):
    return lax.dot_general(a, b, (((1,), (0,)), ((), ())), preferred_element_type=F32)


def mm_nt(a, b):
    return lax.dot_general(a, b, (((1,), (1,)), ((), ())), preferred_element_type=F32)


def mm_tn(a, b):
    return lax.dot_general(a, b, (((0,), (0,)), ((), ())), preferred_element_type=F32)


def pick(selection, source):
    return mm(selection, source).astype(BF)


def norm_parts(values):
    centred = values - jnp.mean(values, axis=-1, keepdims=True)
    spread = jnp.mean(centred * centred, axis=-1, keepdims=True)
    scale = lax.rsqrt(spread + EPSILON)
    return centred * scale, scale


def normed(values, gain):
    return (norm_parts(values)[0] * gain).astype(BF)


def norm_back(values, gain, upstream):
    unit, scale = norm_parts(values)
    inner = upstream * gain
    along = jnp.mean(inner * unit, axis=-1, keepdims=True)
    grad = scale * (inner - jnp.mean(inner, axis=-1, keepdims=True) - unit * along)
    return grad.astype(BF), jnp.sum(upstream * unit, axis=0, keepdims=True)


def lane_head(shape):
    return lax.broadcasted_iota(jnp.int32, shape, 1) // HEAD


def stacked(block):
    heads = lane_head((1, TILE))
    parts = [block * (heads == h).astype(F32).astype(BF) for h in range(TILE // HEAD)]
    return jnp.concatenate(parts, axis=0)


def unstacked(tall):
    heads = lane_head((PAIR, TILE))
    out = tall[:PAIR]
    for h in range(1, TILE // HEAD):
        out = jnp.where(heads == h, tall[h * PAIR : (h + 1) * PAIR], out)
    return out


def soft(queries, keys, bias):
    tall = stacked(queries)
    raised = jnp.exp(mm_nt(tall, keys) * HEAD ** (-0.5) + bias)
    return tall, raised / jnp.sum(raised, axis=-1, keepdims=True)


def tiled_bias(bias):
    return jnp.concatenate([bias] * (TILE // HEAD), axis=0)


def thirds(packed, rows, width, t):
    return (packed[rows, p * width + t * TILE : p * width + (t + 1) * TILE] for p in range(3))


def head_grads(tall, share, above, k, v):
    d_share = mm_nt(above, v).astype(BF).astype(F32)
    along = jnp.sum(d_share * share, axis=-1, keepdims=True)
    d_scores = (share * (d_share - along) * HEAD ** (-0.5)).astype(BF)
    return (
        unstacked(mm(d_scores, k)),
        mm_tn(d_scores, tall),
        mm_tn(share.astype(BF), above),
    )


def put_thirds(out, rows, width, t, grads):
    for p, grad in enumerate(grads):
        at = p * width + t * TILE
        out[rows, at : at + TILE] = grad.astype(BF)


def put_pieces(grad, outs, block, lanes, halves=1):
    cores, xs = len(outs), outs[0].shape[0]
    size = grad.shape[0] // (cores * xs * halves)
    width = grad.shape[1]
    for h in range(halves):
        for c in range(cores):
            for x in range(xs):
                at = ((h * cores + c) * xs + x) * size
                lo = lanes + h * width
                outs[c][x, block * size : (block + 1) * size, lo : lo + width] = grad[
                    at : at + size
                ].astype(BF)


def weight_grad(acts, order, upstream, out, lanes, halves=1):
    side = order.shape[0]
    for block in range(acts.shape[1] // side):
        moved = pick_cols(acts[:, block * side : (block + 1) * side], order)
        put_pieces(mm_tn(moved, upstream), out, block, lanes, halves)


def pick_cols(acts, order):
    return mm(acts, order).astype(BF)


def put_edges(values, edges, outs):
    sent = pick(edges, values)
    at = 0
    for out in outs:
        out[...] = sent[at : at + out.shape[0]]
        at += out.shape[0]


def joined(refs):
    return jnp.concatenate([r[...] for r in refs], axis=0)


def div(value, by):
    return (value * (-(-65536 // by))) >> 16


def mod(value, by):
    return value - div(value, by) * by


def lines(count, at=0):
    return lax.broadcasted_iota(jnp.int32, (count, 1), 0) + at


def one_hot(wanted, width):
    return (wanted == lax.broadcasted_iota(jnp.int32, (wanted.shape[0], width), 1)).astype(F32).astype(BF)


def strip(p, height, breadth, place, row0=0, col0=0):
    r, c = div(p, breadth), mod(p, breadth)
    return jnp.where(p < height * breadth, place(r + row0, c + col0), -1)


def input_edges(tokens, cot, tokens_o, cot_o, t0, t1, t2, c0, c1, c2):
    for source, laid, rows_o, cols_o, corner_o in (
        (tokens, tokens_o, t0, t1, t2),
        (cot, cot_o, c0, c1, c2),
    ):
        rows, cols, width = source.shape
        pad = laid.shape[0] // rows
        blank = jnp.zeros((pad - cols, width), BF)
        parts = []
        for r in range(rows):
            parts += [source[r].astype(F32), blank.astype(F32)]
        whole = jnp.concatenate(parts, axis=0).astype(BF)
        laid[...] = whole
        rows_o[...] = whole[: EDGE * pad]

        def place(r, c, pad=pad):
            return r * pad + c

        for out, height in ((cols_o, rows), (corner_o, EDGE)):
            wanted = strip(lines(out.shape[0]), height, EDGE, place)
            out[...] = pick(one_hot(wanted, whole.shape[0]), whole)


def make_tables(tile, tile3, ranks, depths):
    tile_rows, tile_cols = tile
    three_rows, three_cols = tile3
    pad, pad3 = up16(tile_cols), up16(three_cols)
    size3 = three_rows * pad3
    line2, line3 = tile_cols // WIN, three_cols // WIN
    count2 = line2 * (tile_rows // WIN)
    count3 = line3 * (three_rows // WIN)
    er, ec, ex = up16(EDGE * tile_cols), up16(tile_rows * EDGE), up16(EDGE * EDGE)
    tr, hc = up16(EDGE * three_cols), up16(three_rows * EDGE)
    hr = EDGE * pad3
    main_n, rows_n = tile_rows * pad, EDGE * pad
    n2, n3, n4 = count2 * SLOT, count3 * SLOT, 4 * size3
    rows, xs, cores = ranks

    def window_line(p, line):
        w, t = div(p, SLOT), mod(p, SLOT)
        row = div(w, line) * WIN + div(t, WIN)
        col = mod(w, line) * WIN + mod(t, WIN)
        return t < AREA, row, col

    def window_place(row, col, line):
        w = div(row, WIN) * line + div(col, WIN)
        return w * SLOT + mod(row, WIN) * WIN + mod(col, WIN)

    def in_windows2(r, c):
        return window_place(r, c, line2)

    def in_windows3(r, c):
        return window_place(r, c, line3)

    def in_planes(r, c):
        return (mod(c, 2) * 2 + mod(r, 2)) * size3 + div(r, 2) * pad3 + div(c, 2)

    def pick4(low, right, main, strip_rows, strip_cols, corner):
        return jnp.where(low, jnp.where(right, corner, strip_rows), jnp.where(right, strip_cols, main))

    def ahead(p, line, extent, shifts, place, main, breadth, strip_rows, strip_cols):
        valid, row, col = window_line(p, line)
        r, c = row + shifts[0], col + shifts[1]
        a, b = r - extent[0], c - extent[1]
        at = pick4(
            a >= 0,
            b >= 0,
            place(r, c),
            main + a * breadth + c,
            main + strip_rows + r * EDGE + b,
            main + strip_rows + strip_cols + a * EDGE + b,
        )
        return jnp.where(valid, at, -1)

    def behind(real, r, c, place, main, extent, strip_rows, strip_cols):
        at = pick4(
            r < 0,
            c < 0,
            place(jnp.maximum(r, 0), jnp.maximum(c, 0)),
            main + (r + EDGE) * extent[1] + c,
            main + strip_rows + r * EDGE + c + EDGE,
            main + strip_rows + strip_cols + (r + EDGE) * EDGE + c + EDGE,
        )
        return jnp.where(real, at, -1)

    def edges(p, place, extent, first, sizes):
        h = strip(p, EDGE, extent[1], place, first[0], 0)
        v = strip(p - sizes[0], extent[0], EDGE, place, 0, first[1])
        x = strip(p - sizes[0] - sizes[1], EDGE, EDGE, place, first[0], first[1])
        return jnp.where(p < sizes[0], h, jnp.where(p < sizes[0] + sizes[1], v, x))

    def grid_of(q):
        k, m = div(q, size3), mod(q, size3)
        a, b = div(m, pad3), mod(m, pad3)
        return b < three_cols, 2 * a + mod(k, 2), 2 * b + div(k, 2)

    def body(
        offsets, where, sel_a, tail2, sel_tokens, sel_b, head3, sel3, tail3, sel3b, head2, sel_e,
        sel_out, order2, order3, order_m, bias2, bias3,
    ):
        s0, s1, s2, s3 = (offsets[i] for i in range(4))
        row_rank, x_rank, c_rank = (where[i] for i in range(3))
        col_rank = x_rank * cores + c_rank

        def fill(out, wanted_of, block):
            def step(i, carry):
                at = pl.multiple_of(i * block, block)
                out[pl.ds(at, block), :] = one_hot(wanted_of(lines(block, at)), out.shape[1])
                return carry

            lax.fori_loop(0, out.shape[0] // block, step, 0)

        def in_pad(r, c):
            return r * pad + c

        def in_pad3(r, c):
            return r * pad3 + c

        fill(
            sel_a,
            lambda p: ahead(p, line2, tile, (s0, s1), in_pad, main_n, pad, rows_n, ec),
            64,
        )
        fill(
            tail2,
            lambda p: edges(p, in_windows2, tile, (tile_rows - EDGE, tile_cols - EDGE), (er, ec)),
            64,
        )

        def from_grid(q):
            real, r, c = grid_of(q)
            return jnp.where(real, in_pad(r, c), -1)

        fill(sel_tokens, from_grid, 64)

        def back2(q):
            real, r, c = grid_of(q)
            return behind(real, r - s0, c - s1, in_windows2, n2, tile, er, ec)

        fill(sel_b, back2, 64)

        def head_of_three(p):
            v = strip(p - hr, three_rows, EDGE, in_pad3)
            x = strip(p - hr - hc, EDGE, EDGE, in_pad3)
            return jnp.where(p < hr, p, jnp.where(p < hr + hc, v, x))

        fill(head3, head_of_three, 16)
        fill(
            sel3,
            lambda p: ahead(p, line3, tile3, (s2, s3), in_pad3, size3, pad3, hr, hc),
            64,
        )
        fill(
            tail3,
            lambda p: edges(
                p, in_windows3, tile3, (three_rows - EDGE, three_cols - EDGE), (tr, hc)
            ),
            16,
        )

        def back3(m):
            a, b = div(m, pad3), mod(m, pad3)
            return behind(b < three_cols, a - s2, b - s3, in_windows3, n3, tile3, tr, hc)

        fill(sel3b, back3, 16)
        fill(head2, lambda p: edges(p, in_planes, tile, (0, 0), (er, ec)), 64)
        fill(
            sel_e,
            lambda p: ahead(p, line2, tile, (s0, s1), in_planes, n4, tile_cols, er, ec),
            64,
        )

        def to_grid(g):
            return jnp.where(mod(g, pad) < tile_cols, in_planes(div(g, pad), mod(g, pad)), -1)

        fill(sel_out, to_grid, 64)

        for out, depth, halves in ((order2, depths[0], 1), (order3, depths[1], 1), (order_m, depths[2], 2)):
            side = out.shape[0]
            per_row = depth // rows
            near = side // per_row
            sub = depth // (rows * xs * cores)
            part = sub // halves
            at = lax.broadcasted_iota(jnp.int32, (1, side), 1)
            r = mod(div(at, part), near)
            x = mod(div(at, part * near) + x_rank, xs)
            c = mod(div(at, part * near * xs) + 1 + c_rank, cores)
            h = div(at, part * near * xs * cores)
            source = r * per_row + (x * cores + c) * sub + h * part + mod(at, part)
            lanes = lax.broadcasted_iota(jnp.int32, (side, side), 0)
            out[...] = (lanes == source).astype(F32).astype(BF)

        def label(at, extent, shift):
            return jnp.where(at < extent - WIN, 0, jnp.where(at < extent - shift, 1, 2))

        def marks(p, line, extent, shifts):
            valid, row, col = window_line(p, line)
            r = label(row + row_rank * extent[0], extent[0] * rows, shifts[0])
            c = label(col + col_rank * extent[1], extent[1] * xs * cores, shifts[1])
            near = div(p, SLOT) * 2 + jnp.where(valid, 1, 0)
            return near, jnp.where(valid, r * 3 + c, -1)

        def bias(first, line, extent, shifts):
            near_p, mark_p = marks(lines(PAIR, first), line, extent, shifts)
            across = lax.broadcasted_iota(jnp.int32, (1, PAIR), 1) + first
            near_q, mark_q = marks(across, line, extent, shifts)
            same = jnp.where(mark_p == mark_q, 0.0, MASKED)
            return jnp.where(near_p == near_q, same, APART).astype(F32)

        for g in range(bias2.shape[0]):
            bias2[g] = bias(g * PAIR, line2, tile, (s0, s1))
        bias3[...] = bias(0, line3, tile3, (s2, s3))

    shapes = [
        ((n2, main_n + rows_n + ec + ex), BF),
        ((er + ec + ex, n2), BF),
        ((n4, main_n), BF),
        ((n4, n2 + er + ec + ex), BF),
        ((hr + hc + ex, size3), BF),
        ((n3, size3 + hr + hc + ex), BF),
        ((tr + hc + ex, n3), BF),
        ((size3, n3 + tr + hc + ex), BF),
        ((er + ec + ex, n4), BF),
        ((n2, n4 + er + ec + ex), BF),
        ((main_n, n4), BF),
        ((256, 256), BF),
        ((256, 256), BF),
        ((256, 256), BF),
        ((n2 // PAIR, PAIR, PAIR), F32),
        ((PAIR, PAIR), F32),
    ]
    return body, shapes


def two_forward(
    t0, t1, t2, t3, gain, qkv, proj, sel, bias, edges, rolled_o, packed_o, mixed_o, wins_o, e0, e1, e2
):
    tokens = pick(sel[...], joined((t0, t1, t2, t3)))
    rolled = normed(tokens.astype(F32), gain[...])
    rolled_o[...] = rolled
    packed_o[...] = mm(rolled, qkv[...]).astype(BF)
    width = rolled.shape[1]
    for g in range(packed_o.shape[0] // PAIR):
        rows = slice(g * PAIR, (g + 1) * PAIR)
        mask = tiled_bias(bias[g])
        for t in range(width // TILE):
            q, k, v = thirds(packed_o, rows, width, t)
            share = soft(q, k, mask)[1].astype(BF)
            mixed_o[rows, t * TILE : (t + 1) * TILE] = unstacked(mm(share, v)).astype(BF)
    projected = mm(mixed_o[...], proj[...]).astype(BF)
    wins_o[...] = projected
    put_edges(projected, edges[...], (e0, e1, e2))


def merge_forward(
    tokens, w0, w1, w2, w3, sel_tokens, sel_back, gain, weight, gain3, edges,
    two_o, tokens_o, norm_o, merged_o, normed_o, e0, e1, e2,
):
    laid = pick(sel_tokens[...], tokens[...])
    back = pick(sel_back[...], joined((w0, w1, w2, w3)))
    two = (laid.astype(F32) + back.astype(F32)).astype(BF)
    tokens_o[...] = laid
    size = two.shape[0] // 4
    wide = jnp.concatenate([two[k * size : (k + 1) * size] for k in range(4)], axis=1)
    two_o[...] = wide
    merged_norm = normed(wide.astype(F32), gain[...])
    norm_o[...] = merged_norm
    merged = mm(merged_norm, weight[...]).astype(BF)
    merged_o[...] = merged
    three = normed(merged.astype(F32), gain3[...])
    normed_o[...] = three
    put_edges(three, edges[...], (e0, e1, e2))


def three_both(
    n0, n1, n2, n3, c0, c1, c2, c3, qkv, proj, sel, bias, edges,
    both_o, rolled_o, above_o, mixed, d_packed, e0, e1, e2, packed,
):
    rolled = pick(sel[...], joined((n0, n1, n2, n3)))
    above = pick(sel[...], joined((c0, c1, c2, c3)))
    rolled_o[...] = rolled
    above_o[...] = above
    width = rolled.shape[1]
    packed[...] = mm(rolled, qkv[...]).astype(BF)
    d_mixed = mm_nt(above, proj[...]).astype(BF)
    mask = tiled_bias(bias[...])
    rows = slice(0, PAIR)
    for t in range(width // TILE):
        lanes = slice(t * TILE, (t + 1) * TILE)
        q, k, v = thirds(packed, rows, width, t)
        tall, share = soft(q, k, mask)
        mixed[:, lanes] = unstacked(mm(share.astype(BF), v)).astype(BF)
        put_thirds(
            d_packed, rows, width, t, head_grads(tall, share, stacked(d_mixed[:, lanes]), k, v)
        )
    projected = mm(mixed[...], proj[...]).astype(BF)
    d_rolled = mm_nt(d_packed[...], qkv[...]).astype(BF)
    both = jnp.concatenate([projected, d_rolled], axis=1)
    both_o[...] = both
    put_edges(both, edges[...], (e0, e1, e2))


def three_grads(rolled, above, mixed, d_packed, order, send_o, keep_o):
    outs = (send_o, keep_o)
    weight_grad(rolled[...], order[...], d_packed[...], outs, 0)
    weight_grad(mixed[...], order[...], above[...], outs, 3 * rolled.shape[1])


def merge_backward(
    b0, b1, b2, b3, merged, cot, two, sel_back, gain3, gain, weight, edges,
    out_o, d_two_o, d_rows_o, gm_o, g3_o, e0, e1, e2,
):
    back = pick(sel_back[...], joined((b0, b1, b2, b3)))
    width = merged.shape[1]
    base = merged[...].astype(F32)
    out = base + back[:, :width].astype(F32)
    rows, cols = out_o.shape[:2]
    pad = out.shape[0] // rows
    for r in range(rows):
        out_o[r] = out[r * pad : r * pad + cols].astype(BF)
    d_normed = back[:, width:].astype(F32)
    d_merged, g3 = norm_back(base, gain3[...], d_normed)
    g3_o[...] = g3
    d_rows = (cot[...].astype(F32) + d_merged.astype(F32)).astype(BF)
    d_rows_o[...] = d_rows
    d_norm = mm_nt(d_rows, weight[...]).astype(BF).astype(F32)
    d_wide, gm = norm_back(two[...].astype(F32), gain[...], d_norm)
    gm_o[...] = gm
    quarter = d_wide.shape[1] // 4
    d_two = jnp.concatenate([d_wide[:, k * quarter : (k + 1) * quarter] for k in range(4)], axis=0)
    d_two_o[...] = d_two
    put_edges(d_two, edges[...], (e0, e1, e2))


def merge_grads(norm, d_rows, order, send_o, keep_o):
    weight_grad(norm[...], order[...], d_rows[...], (send_o, keep_o), 0, halves=2)


def two_backward(
    d0, d1, d2, d3, mixed, packed, rolled, qkv, proj, gain, sel, bias, edges, order, gm, g3,
    wins_o, send_o, keep_o, e0, e1, e2, d_packed, d_mixed,
):
    above = pick(sel[...], joined((d0, d1, d2, d3)))
    width = above.shape[1]
    d_mixed[...] = mm_nt(above, proj[...]).astype(BF)

    def step(g, carry):
        rows = pl.ds(pl.multiple_of(g * PAIR, PAIR), PAIR)
        mask = tiled_bias(bias[g])
        for t in range(width // TILE):
            q, k, v = thirds(packed, rows, width, t)
            tall, share = soft(q, k, mask)
            given = stacked(d_mixed[rows, t * TILE : (t + 1) * TILE])
            put_thirds(d_packed, rows, width, t, head_grads(tall, share, given, k, v))
        return carry

    lax.fori_loop(0, packed.shape[0] // PAIR, step, 0)
    d_rolled = mm_nt(d_packed[...], qkv[...]).astype(BF)
    wins_o[...] = d_rolled
    put_edges(d_rolled, edges[...], (e0, e1, e2))
    outs = (send_o, keep_o)
    weight_grad(rolled[...], order[...], d_packed[...], outs, 0)
    weight_grad(mixed[...], order[...], above, outs, 3 * width)
    g2 = jnp.sum(d_rolled.astype(F32) * rolled[...].astype(F32), axis=0, keepdims=True) / gain[...]
    blank = jnp.zeros((1, width), F32)
    second = jnp.concatenate([g3[...], g2, blank], axis=1)
    line = lax.broadcasted_iota(jnp.int32, (16, 4 * width), 0)
    gains = jnp.where(line == 0, gm[...], jnp.where(line == 1, second, 0.0)).astype(BF)
    for out in outs:
        xs, rows = out.shape[:2]
        for x in range(xs):
            out[x, rows - 16 :, :] = gains


def tokens_backward(w0, w1, w2, w3, tokens, d_two, gain, sel_back, sel_out, out_o):
    d_normed = pick(sel_back[...], joined((w0, w1, w2, w3)))
    d_norm, _ = norm_back(tokens[...].astype(F32), gain[...], d_normed.astype(F32))
    total = (d_two[...].astype(F32) + d_norm.astype(F32)).astype(BF)
    laid = pick(sel_out[...], total)
    rows, cols = out_o.shape[:2]
    pad = laid.shape[0] // rows
    for r in range(rows):
        out_o[r] = laid[r * pad : r * pad + cols]


def pair_sum(keep, got, *outs):
    for x, out in enumerate(outs):
        out[...] = (keep[x].astype(F32) + got[x].astype(F32)).astype(BF)


def line_added(parts):
    parts = [p[...].astype(F32) for p in parts]
    while len(parts) > 1:
        half = len(parts) // 2
        parts = [parts[j] + parts[j + half] for j in range(half)]
    return parts[0]


def put_blocks(value, out, at):
    rows, sub = out.shape[:2]
    for r in range(rows):
        out[r, :, at : at + value.shape[1]] = value[r * sub : (r + 1) * sub].astype(BF)


def line_sum(*refs):
    *held, out = refs
    put_blocks(line_added(held), out, 0)


def line_sum_late(*refs):
    *held, out = refs
    count = len(held) // 2
    rows, sub = out.shape[:2]
    first = line_added(held[:count])
    second = line_added(held[count:]).astype(BF)
    share = second.shape[0] - 16
    part = share // rows
    p = lines(rows * sub)
    r, j = div(p, sub), mod(p, sub)
    wanted = jnp.where(j < part, r * part + j, share + j - part)
    put_blocks(first, out, 0)
    put_blocks(mm(one_hot(wanted, second.shape[0]), second), out, first.shape[1])


def call(body, outs, args, flops, scratch=(), scalars=0):
    smem, vmem = (pl.BlockSpec(memory_space=m) for m in (pltpu.SMEM, pltpu.VMEM))
    return pl.pallas_call(
        body,
        in_specs=[smem] * scalars + [vmem] * (len(args) - scalars),
        out_shape=[jax.ShapeDtypeStruct(shape, kind) for shape, kind in outs],
        scratch_shapes=[pltpu.VMEM(shape, kind) for shape, kind in scratch],
        cost_estimate=pl.CostEstimate(flops=flops, transcendentals=0, bytes_accessed=4 << 20),
        compiler_params=pltpu.CompilerParams(vmem_limit_bytes=8 << 20),
    )(*args)


def moved(value, axis, by):
    count = lax.axis_size(axis)
    return lax.ppermute(value, axis, [(i, (i + by) % count) for i in range(count)])


def moved_across(value, by):
    rows, cols = lax.axis_size("rows"), lax.axis_size(COLS)
    pairs = [
        (i * cols + j, ((i + by) % rows) * cols + (j + by) % cols)
        for i in range(rows)
        for j in range(cols)
    ]
    return lax.ppermute(value, ROWS_COLS, pairs)


def to_neighbours(pieces, by):
    rows, cols, corner = pieces
    return moved_across(corner, by), moved(rows, "rows", by), moved(cols, COLS, by)


def exchanged(pieces, by):
    corner, rows, cols = to_neighbours(pieces, by)
    return rows, cols, corner


def core_sum(send, keep):
    got = moved(send, "cols_1", 1)
    shape = (keep.shape[1:], BF)
    return call(pair_sum, [shape] * keep.shape[0], (keep, got), 1 << 26)


def line_parts(blocks):
    return [blocks[0]] + [moved(blocks[j], "cols_0", j) for j in range(1, len(blocks))]


def spread_sum(body, held, shape):
    (blocks,) = call(body, [(shape, BF)], held, 1 << 26)
    spread = lax.all_to_all(blocks, "rows", 0, 0)
    return jnp.sum(spread.astype(F32), axis=0)


def on_device(
    tokens,
    cotangent,
    shift_offsets,
    norm2_gain,
    qkv2,
    proj2,
    merge_gain,
    merge_weight,
    norm3_gain,
    qkv3,
    proj3,
):
    tile_rows, tile_cols, narrow = tokens.shape
    three_rows, three_cols, wide = cotangent.shape
    ranks = tuple(lax.axis_size(a) for a in ROWS_COLS)
    rows, xs, cores = ranks
    pad, pad3 = up16(tile_cols), up16(three_cols)
    size3 = three_rows * pad3
    n2 = (tile_rows // WIN) * (tile_cols // WIN) * SLOT
    n3 = (three_rows // WIN) * (three_cols // WIN) * SLOT
    n4 = 4 * size3
    er, ec, ex = up16(EDGE * tile_cols), up16(tile_rows * EDGE), up16(EDGE * EDGE)
    hr, tr, hc = EDGE * pad3, up16(EDGE * three_cols), up16(three_rows * EDGE)
    gain2, gain_m, gain3 = norm2_gain[None], merge_gain[None], norm3_gain[None]

    tokens_p, cot_p, *pieces = call(
        input_edges,
        [
            ((tile_rows * pad, narrow), BF),
            ((size3, wide), BF),
            ((EDGE * pad, narrow), BF),
            ((ec, narrow), BF),
            ((ex, narrow), BF),
            ((hr, wide), BF),
            ((hc, wide), BF),
            ((ex, wide), BF),
        ],
        (tokens, cotangent),
        1 << 28,
    )
    token_pieces = exchanged(pieces[:3], -1)
    cot_pieces = exchanged(pieces[3:], -1)
    where = jnp.stack([lax.axis_index(a) for a in ROWS_COLS]).astype(jnp.int32)
    tables, shapes = make_tables(
        (tile_rows, tile_cols), (three_rows, three_cols), ranks, (narrow, wide, 4 * narrow)
    )
    (
        sel_a, tail2, sel_tokens, sel_b, head3, sel3, tail3, sel3b, head2, sel_e, sel_out,
        order2, order3, order_m, bias2, bias3,
    ) = call(tables, shapes, (shift_offsets, where), 1 << 28, scalars=2)

    rolled, packed, mixed, wins, *edges = call(
        two_forward,
        [
            ((n2, narrow), BF),
            ((n2, 3 * narrow), BF),
            ((n2, narrow), BF),
            ((n2, narrow), BF),
            ((er, narrow), BF),
            ((ec, narrow), BF),
            ((ex, narrow), BF),
        ],
        (tokens_p, *token_pieces, gain2, qkv2, proj2, sel_a, bias2, tail2),
        1 << 30,
    )
    back = exchanged(edges, 1)
    two, tokens_q, merged_norm, merged, normed3, *edges = call(
        merge_forward,
        [
            ((size3, 4 * narrow), BF),
            ((n4, narrow), BF),
            ((size3, 4 * narrow), BF),
            ((size3, wide), BF),
            ((size3, wide), BF),
            ((hr, wide), BF),
            ((hc, wide), BF),
            ((ex, wide), BF),
        ],
        (tokens_p, wins, *back, sel_tokens, sel_b, gain_m, merge_weight, gain3, head3),
        1 << 30,
    )
    ahead = exchanged(edges, -1)
    both, rolled3, above3, mixed3, d_packed3, *edges = call(
        three_both,
        [
            ((n3, 2 * wide), BF),
            ((n3, wide), BF),
            ((n3, wide), BF),
            ((n3, wide), BF),
            ((n3, 3 * wide), BF),
            ((tr, 2 * wide), BF),
            ((hc, 2 * wide), BF),
            ((ex, 2 * wide), BF),
        ],
        (normed3, *ahead, cot_p, *cot_pieces, qkv3, proj3, sel3, bias3, tail3),
        1 << 30,
        scratch=[((n3, 3 * wide), BF)],
    )
    back = exchanged(edges, 1)
    share3 = wide // (xs * cores)
    send, keep = call(
        three_grads,
        [((xs, share3, 4 * wide), BF)] * 2,
        (rolled3, above3, mixed3, d_packed3, order3),
        1 << 30,
    )
    sum_a = core_sum(send, keep)
    merged_out, d_two, d_rows, grad_m, grad_3, *edges = call(
        merge_backward,
        [
            ((three_rows, three_cols, wide), BF),
            ((n4, narrow), BF),
            ((size3, wide), BF),
            ((1, 4 * narrow), F32),
            ((1, wide), F32),
            ((er, narrow), BF),
            ((ec, narrow), BF),
            ((ex, narrow), BF),
        ],
        (both, *back, merged, cot_p, two, sel3b, gain3, gain_m, merge_weight, head2),
        1 << 30,
    )
    ahead = exchanged(edges, -1)
    send, keep = call(
        merge_grads, [((xs, share3, 2 * wide), BF)] * 2, (merged_norm, d_rows, order_m), 1 << 30
    )
    sum_b = core_sum(send, keep)
    share2 = narrow // (xs * cores)
    wins, send, keep, *edges = call(
        two_backward,
        [
            ((n2, narrow), BF),
            ((xs, share2 + 16, 4 * narrow), BF),
            ((xs, share2 + 16, 4 * narrow), BF),
            ((er, narrow), BF),
            ((ec, narrow), BF),
            ((ex, narrow), BF),
        ],
        (
            d_two, *ahead, mixed, packed, rolled, qkv2, proj2, gain2, sel_e, bias2, tail2,
            order2, grad_m, grad_3,
        ),
        1 << 30,
        scratch=[((n2, 3 * narrow), BF), ((n2, narrow), BF)],
    )
    back = exchanged(edges, 1)
    sum_c = core_sum(send, keep)
    (tokens_grad,) = call(
        tokens_backward,
        [((tile_rows, tile_cols, narrow), BF)],
        (wins, *back, tokens_q, d_two, gain2, sel_b, sel_out),
        1 << 30,
    )

    sub = wide // (rows * xs * cores)
    early = spread_sum(line_sum, line_parts(sum_a), (rows, sub, 4 * wide))
    late = spread_sum(
        line_sum_late, line_parts(sum_b) + line_parts(sum_c), (rows, sub, 2 * wide + 4 * narrow)
    )
    chunk3 = early.astype(BF)
    merge_chunk = late[:, : 2 * wide].astype(BF)
    late = late[:, 2 * wide :]
    sub2 = narrow // (rows * xs * cores)
    gain_sums = jnp.concatenate(
        [late[sub2 + 1, wide : wide + narrow], late[sub2], late[sub2 + 1, :wide]]
    )
    chunk2 = late[:sub2].astype(BF)
    halves = [merge_chunk[:, h * wide : (h + 1) * wide] for h in range(2)]
    return (
        merged_out,
        tokens_grad,
        gain_sums,
        chunk2[:, : 3 * narrow].reshape(-1),
        chunk2[:, 3 * narrow :].reshape(-1),
        jnp.concatenate(halves, axis=0).reshape(-1),
        chunk3[:, : 3 * wide].reshape(-1),
        chunk3[:, 3 * wide :].reshape(-1),
    )


def solution(mesh):
    cores = 2
    split = Mesh(
        mesh.devices.reshape(
            mesh.shape["groups"], mesh.shape["rows"], mesh.shape["cols"] // cores, cores
        ),
        ("groups", "rows", "cols_0", "cols_1"),
    )
    tiles = P(("groups", "rows"), COLS, None)
    flat = P(GROUPS_ROWS_COLS)


    return jax.shard_map(
        on_device,
        mesh=split,
        in_specs=(tiles, tiles) + (P(),) * 9,
        out_specs=(tiles, tiles, P("groups"), flat, flat, flat, flat, flat),
        check_vma=False,
    )
```

```python
import jax
import jax.numpy as jnp
from jax import lax
from jax.experimental import pallas as pl
from jax.experimental.pallas import tpu as pltpu
from jax.sharding import Mesh
from jax.sharding import PartitionSpec as P


WIN = 7
AREA = WIN * WIN
SLOT = 64
PAIR = 2 * SLOT
TILE = 128
HEAD = 32
EDGE = WIN - 1
NEAR = 4
COLS = ("cols_0", "cols_1")
ROWS_COLS = ("rows", "cols_0", "cols_1")
GROUPS_ROWS_COLS = ("groups", "rows", "cols_0", "cols_1")

EPSILON = 1e-05
MASKED = -100.0
APART = -1e30
BF = jnp.bfloat16
F32 = jnp.float32


def up16(count):
    return -(-count // 16) * 16


def mm(a, b):
    return lax.dot_general(a, b, (((1,), (0,)), ((), ())), preferred_element_type=F32)


def mm_nt(a, b):
    return lax.dot_general(a, b, (((1,), (1,)), ((), ())), preferred_element_type=F32)


def mm_tn(a, b):
    return lax.dot_general(a, b, (((0,), (0,)), ((), ())), preferred_element_type=F32)


def pick(selection, source):
    return mm(selection, source).astype(BF)


def norm_parts(values):
    centred = values - jnp.mean(values, axis=-1, keepdims=True)
    spread = jnp.mean(centred * centred, axis=-1, keepdims=True)
    scale = lax.rsqrt(spread + EPSILON)
    return centred * scale, scale


def normed(values, gain):
    return (norm_parts(values)[0] * gain).astype(BF)


def norm_back(values, gain, upstream):
    unit, scale = norm_parts(values)
    inner = upstream * gain
    along = jnp.mean(inner * unit, axis=-1, keepdims=True)
    grad = scale * (inner - jnp.mean(inner, axis=-1, keepdims=True) - unit * along)
    return grad.astype(BF), jnp.sum(upstream * unit, axis=0, keepdims=True)


def lane_head(shape):
    return lax.broadcasted_iota(jnp.int32, shape, 1) // HEAD


def stacked(block):
    heads = lane_head((1, TILE))
    parts = [block * (heads == h).astype(F32).astype(BF) for h in range(TILE // HEAD)]
    return jnp.concatenate(parts, axis=0)


def unstacked(tall):
    heads = lane_head((PAIR, TILE))
    out = tall[:PAIR]
    for h in range(1, TILE // HEAD):
        out = jnp.where(heads == h, tall[h * PAIR : (h + 1) * PAIR], out)
    return out


def soft(queries, keys, bias):
    tall = stacked(queries)
    raised = jnp.exp(mm_nt(tall, keys) * HEAD ** (-0.5) + bias)
    return tall, raised / jnp.sum(raised, axis=-1, keepdims=True)


def tiled_bias(bias):
    return jnp.concatenate([bias] * (TILE // HEAD), axis=0)


def tile_at(start):
    return pl.ds(pl.multiple_of(start, TILE), TILE)


def thirds(packed, rows, width, t):
    return (packed[rows, tile_at(p * width + t * TILE)] for p in range(3))


def head_grads(tall, share, above, k, v):
    d_share = mm_nt(above, v).astype(BF).astype(F32)
    along = jnp.sum(d_share * share, axis=-1, keepdims=True)
    d_scores = (share * (d_share - along) * HEAD ** (-0.5)).astype(BF)
    return (
        unstacked(mm(d_scores, k)),
        mm_tn(d_scores, tall),
        mm_tn(share.astype(BF), above),
    )


def put_thirds(out, rows, width, t, grads):
    for p, grad in enumerate(grads):
        out[rows, tile_at(p * width + t * TILE)] = grad.astype(BF)


def put_pieces(grad, outs, block, lanes, halves=1):
    cores, xs = len(outs), outs[0].shape[0]
    size = grad.shape[0] // (cores * xs * halves)
    width = grad.shape[1]
    rows = pl.ds(pl.multiple_of(block * size, size), size)
    for h in range(halves):
        for c in range(cores):
            for x in range(xs):
                at = ((h * cores + c) * xs + x) * size
                lo = lanes + h * width
                outs[c][x, rows, lo : lo + width] = grad[at : at + size].astype(BF)


def weight_grad(acts, order, upstream, outs, lanes, halves=1):
    side = order.shape[0]

    def step(block, carry):
        cols = pl.ds(pl.multiple_of(block * side, side), side)
        moved_cols = pick_cols(acts[:, cols], order)
        put_pieces(mm_tn(moved_cols, upstream), outs, block, lanes, halves)
        return carry

    lax.fori_loop(0, acts.shape[1] // side, step, 0)


def pick_cols(acts, order):
    return mm(acts, order).astype(BF)


def put_edges(values, edges, outs):
    sent = pick(edges, values)
    at = 0
    for out in outs:
        out[...] = sent[at : at + out.shape[0]]
        at += out.shape[0]


def joined(refs):
    return jnp.concatenate([r[...] for r in refs], axis=0)


def div(value, by):
    return (value * (-(-65536 // by))) >> 16


def mod(value, by):
    return value - div(value, by) * by


def lines(count, at=0):
    return lax.broadcasted_iota(jnp.int32, (count, 1), 0) + at


def one_hot(wanted, width):
    return (wanted == lax.broadcasted_iota(jnp.int32, (wanted.shape[0], width), 1)).astype(F32).astype(BF)


def strip(p, height, breadth, place, row0=0, col0=0):
    r, c = div(p, breadth), mod(p, breadth)
    return jnp.where(p < height * breadth, place(r + row0, c + col0), -1)


def input_edges(source, laid, rows_o, cols_o, corner_o):
    rows, cols, width = source.shape
    pad = laid.shape[0] // rows
    blank = jnp.zeros((pad - cols, width), F32)
    parts = []
    for r in range(rows):
        parts += [source[r].astype(F32), blank]
    whole = jnp.concatenate(parts, axis=0).astype(BF)
    laid[...] = whole
    rows_o[...] = whole[: EDGE * pad]

    def place(r, c):
        return r * pad + c

    for out, height in ((cols_o, rows), (corner_o, EDGE)):
        wanted = strip(lines(out.shape[0]), height, EDGE, place)
        out[...] = pick(one_hot(wanted, whole.shape[0]), whole)


def make_tables(tile, tile3, ranks, depths):
    tile_rows, tile_cols = tile
    three_rows, three_cols = tile3
    pad, pad3 = up16(tile_cols), up16(three_cols)
    size3 = three_rows * pad3
    line2, line3 = tile_cols // WIN, three_cols // WIN
    count2 = line2 * (tile_rows // WIN)
    count3 = line3 * (three_rows // WIN)
    er, ec, ex = up16(EDGE * tile_cols), up16(tile_rows * EDGE), up16(EDGE * EDGE)
    tr, hc = up16(EDGE * three_cols), up16(three_rows * EDGE)
    hr = EDGE * pad3
    main_n, rows_n = tile_rows * pad, EDGE * pad
    n2, n3, n4 = count2 * SLOT, count3 * SLOT, 4 * size3
    rows, xs, cores = ranks

    def window_line(p, line):
        w, t = div(p, SLOT), mod(p, SLOT)
        row = div(w, line) * WIN + div(t, WIN)
        col = mod(w, line) * WIN + mod(t, WIN)
        return t < AREA, row, col

    def window_place(row, col, line):
        w = div(row, WIN) * line + div(col, WIN)
        return w * SLOT + mod(row, WIN) * WIN + mod(col, WIN)

    def in_windows2(r, c):
        return window_place(r, c, line2)

    def in_windows3(r, c):
        return window_place(r, c, line3)

    def in_planes(r, c):
        return (mod(c, 2) * 2 + mod(r, 2)) * size3 + div(r, 2) * pad3 + div(c, 2)

    def pick4(low, right, main, strip_rows, strip_cols, corner):
        return jnp.where(low, jnp.where(right, corner, strip_rows), jnp.where(right, strip_cols, main))

    def ahead(p, line, extent, shifts, place, main, breadth, strip_rows, strip_cols):
        valid, row, col = window_line(p, line)
        r, c = row + shifts[0], col + shifts[1]
        a, b = r - extent[0], c - extent[1]
        at = pick4(
            a >= 0,
            b >= 0,
            place(r, c),
            main + a * breadth + c,
            main + strip_rows + r * EDGE + b,
            main + strip_rows + strip_cols + a * EDGE + b,
        )
        return jnp.where(valid, at, -1)

    def behind(real, r, c, place, main, extent, strip_rows, strip_cols):
        at = pick4(
            r < 0,
            c < 0,
            place(jnp.maximum(r, 0), jnp.maximum(c, 0)),
            main + (r + EDGE) * extent[1] + c,
            main + strip_rows + r * EDGE + c + EDGE,
            main + strip_rows + strip_cols + (r + EDGE) * EDGE + c + EDGE,
        )
        return jnp.where(real, at, -1)

    def edges(p, place, extent, first, sizes):
        h = strip(p, EDGE, extent[1], place, first[0], 0)
        v = strip(p - sizes[0], extent[0], EDGE, place, 0, first[1])
        x = strip(p - sizes[0] - sizes[1], EDGE, EDGE, place, first[0], first[1])
        return jnp.where(p < sizes[0], h, jnp.where(p < sizes[0] + sizes[1], v, x))

    def grid_of(q):
        k, m = div(q, size3), mod(q, size3)
        a, b = div(m, pad3), mod(m, pad3)
        return b < three_cols, 2 * a + mod(k, 2), 2 * b + div(k, 2)

    def fill(out, wanted_of, block):
        def step(i, carry):
            at = pl.multiple_of(i * block, block)
            out[pl.ds(at, block), :] = one_hot(wanted_of(lines(block, at)), out.shape[1])
            return carry

        lax.fori_loop(0, out.shape[0] // block, step, 0)

    def in_pad(r, c):
        return r * pad + c

    def in_pad3(r, c):
        return r * pad3 + c

    def label(at, extent, shift):
        return jnp.where(at < extent - WIN, 0, jnp.where(at < extent - shift, 1, 2))

    def bias(where, first, line, extent, shifts):
        row_rank, x_rank, c_rank = (where[i] for i in range(3))
        col_rank = x_rank * cores + c_rank

        def marks(p):
            valid, row, col = window_line(p, line)
            r = label(row + row_rank * extent[0], extent[0] * rows, shifts[0])
            c = label(col + col_rank * extent[1], extent[1] * xs * cores, shifts[1])
            near = div(p, SLOT) * 2 + jnp.where(valid, 1, 0)
            return near, jnp.where(valid, r * 3 + c, -1)

        near_p, mark_p = marks(lines(PAIR, first))
        near_q, mark_q = marks(lax.broadcasted_iota(jnp.int32, (1, PAIR), 1) + first)
        same = jnp.where(mark_p == mark_q, 0.0, MASKED)
        return jnp.where(near_p == near_q, same, APART).astype(F32)

    def early(offsets, where, sel_a, tail2, sel_tokens, sel_b, head3, bias2):
        s0, s1 = offsets[0], offsets[1]
        fill(
            sel_a,
            lambda p: ahead(p, line2, tile, (s0, s1), in_pad, main_n, pad, rows_n, ec),
            32,
        )
        fill(
            tail2,
            lambda p: edges(p, in_windows2, tile, (tile_rows - EDGE, tile_cols - EDGE), (er, ec)),
            32,
        )

        def from_grid(q):
            real, r, c = grid_of(q)
            return jnp.where(real, in_pad(r, c), -1)

        fill(sel_tokens, from_grid, 32)

        def back2(q):
            real, r, c = grid_of(q)
            return behind(real, r - s0, c - s1, in_windows2, n2, tile, er, ec)

        fill(sel_b, back2, 32)

        def head_of_three(p):
            v = strip(p - hr, three_rows, EDGE, in_pad3)
            x = strip(p - hr - hc, EDGE, EDGE, in_pad3)
            return jnp.where(p < hr, p, jnp.where(p < hr + hc, v, x))

        fill(head3, head_of_three, 16)
        for g in range(bias2.shape[0]):
            bias2[g] = bias(where, g * PAIR, line2, tile, (s0, s1))

    def late(
        offsets, where, sel3, tail3, sel3b, head2, sel_e, sel_out, order2, order3, order_m, bias3
    ):
        s0, s1, s2, s3 = (offsets[i] for i in range(4))
        x_rank, c_rank = where[1], where[2]
        fill(
            sel3,
            lambda p: ahead(p, line3, tile3, (s2, s3), in_pad3, size3, pad3, hr, hc),
            32,
        )
        fill(
            tail3,
            lambda p: edges(
                p, in_windows3, tile3, (three_rows - EDGE, three_cols - EDGE), (tr, hc)
            ),
            16,
        )

        def back3(m):
            a, b = div(m, pad3), mod(m, pad3)
            return behind(b < three_cols, a - s2, b - s3, in_windows3, n3, tile3, tr, hc)

        fill(sel3b, back3, 16)
        fill(head2, lambda p: edges(p, in_planes, tile, (0, 0), (er, ec)), 32)
        fill(
            sel_e,
            lambda p: ahead(p, line2, tile, (s0, s1), in_planes, n4, tile_cols, er, ec),
            32,
        )

        def to_grid(g):
            return jnp.where(mod(g, pad) < tile_cols, in_planes(div(g, pad), mod(g, pad)), -1)

        fill(sel_out, to_grid, 32)

        for out, depth, halves in ((order2, depths[0], 1), (order3, depths[1], 1), (order_m, depths[2], 2)):
            side = out.shape[0]
            per_row = depth // rows
            near = side // per_row
            sub = depth // (rows * xs * cores)
            part = sub // halves
            at = lax.broadcasted_iota(jnp.int32, (1, side), 1)
            r = mod(div(at, part), near)
            x = mod(div(at, part * near) + x_rank, xs)
            c = mod(div(at, part * near * xs) + 1 + c_rank, cores)
            h = div(at, part * near * xs * cores)
            source = r * per_row + (x * cores + c) * sub + h * part + mod(at, part)
            lanes = lax.broadcasted_iota(jnp.int32, (side, side), 0)
            out[...] = (lanes == source).astype(F32).astype(BF)

        bias3[...] = bias(where, 0, line3, tile3, (s2, s3))

    early_shapes = [
        ((n2, main_n + rows_n + ec + ex), BF),
        ((er + ec + ex, n2), BF),
        ((n4, main_n), BF),
        ((n4, n2 + er + ec + ex), BF),
        ((hr + hc + ex, size3), BF),
        ((n2 // PAIR, PAIR, PAIR), F32),
    ]
    late_shapes = [
        ((n3, size3 + hr + hc + ex), BF),
        ((tr + hc + ex, n3), BF),
        ((size3, n3 + tr + hc + ex), BF),
        ((er + ec + ex, n4), BF),
        ((n2, n4 + er + ec + ex), BF),
        ((main_n, n4), BF),
        ((256, 256), BF),
        ((256, 256), BF),
        ((256, 256), BF),
        ((PAIR, PAIR), F32),
    ]
    return early, early_shapes, late, late_shapes


def two_forward(
    t0, t1, t2, t3, gain, qkv, proj, sel, bias, edges, rolled_o, packed_o, mixed_o, wins_o, e0, e1, e2
):
    tokens = pick(sel[...], joined((t0, t1, t2, t3)))
    rolled = normed(tokens.astype(F32), gain[...])
    rolled_o[...] = rolled
    packed_o[...] = mm(rolled, qkv[...]).astype(BF)
    width = rolled.shape[1]

    def step(g, carry):
        rows = pl.ds(pl.multiple_of(g * PAIR, PAIR), PAIR)
        mask = tiled_bias(bias[g])
        for t in range(width // TILE):
            q, k, v = thirds(packed_o, rows, width, t)
            share = soft(q, k, mask)[1].astype(BF)
            mixed_o[rows, tile_at(t * TILE)] = unstacked(mm(share, v)).astype(BF)
        return carry

    lax.fori_loop(0, packed_o.shape[0] // PAIR, step, 0)
    projected = mm(mixed_o[...], proj[...]).astype(BF)
    wins_o[...] = projected
    put_edges(projected, edges[...], (e0, e1, e2))


def merge_forward(
    tokens, w0, w1, w2, w3, sel_tokens, sel_back, gain, weight, gain3, edges,
    two_o, tokens_o, norm_o, merged_o, normed_o, e0, e1, e2,
):
    laid = pick(sel_tokens[...], tokens[...])
    back = pick(sel_back[...], joined((w0, w1, w2, w3)))
    two = (laid.astype(F32) + back.astype(F32)).astype(BF)
    tokens_o[...] = laid
    size = two.shape[0] // 4
    wide = jnp.concatenate([two[k * size : (k + 1) * size] for k in range(4)], axis=1)
    two_o[...] = wide
    merged_norm = normed(wide.astype(F32), gain[...])
    norm_o[...] = merged_norm
    merged = mm(merged_norm, weight[...]).astype(BF)
    merged_o[...] = merged
    three = normed(merged.astype(F32), gain3[...])
    normed_o[...] = three
    put_edges(three, edges[...], (e0, e1, e2))


def three_both(
    n0, n1, n2, n3, c0, c1, c2, c3, qkv, proj, sel, bias, edges,
    both_o, rolled_o, above_o, mixed, d_packed, e0, e1, e2, packed, d_mixed,
):
    rolled = pick(sel[...], joined((n0, n1, n2, n3)))
    above = pick(sel[...], joined((c0, c1, c2, c3)))
    rolled_o[...] = rolled
    above_o[...] = above
    width = rolled.shape[1]
    packed[...] = mm(rolled, qkv[...]).astype(BF)
    d_mixed[...] = mm_nt(above, proj[...]).astype(BF)
    mask = tiled_bias(bias[...])
    rows = slice(0, PAIR)

    def step(i, carry):
        for t in (2 * i, 2 * i + 1):
            lanes = tile_at(t * TILE)
            q, k, v = thirds(packed, rows, width, t)
            tall, share = soft(q, k, mask)
            mixed[rows, lanes] = unstacked(mm(share.astype(BF), v)).astype(BF)
            given = stacked(d_mixed[rows, lanes])
            put_thirds(d_packed, rows, width, t, head_grads(tall, share, given, k, v))
        return carry

    lax.fori_loop(0, width // (2 * TILE), step, 0)
    projected = mm(mixed[...], proj[...]).astype(BF)
    d_rolled = mm_nt(d_packed[...], qkv[...]).astype(BF)
    both = jnp.concatenate([projected, d_rolled], axis=1)
    both_o[...] = both
    put_edges(both, edges[...], (e0, e1, e2))


def three_grads(rolled, above, mixed, d_packed, order, send_o, keep_o):
    outs = (send_o, keep_o)
    weight_grad(rolled, order[...], d_packed[...], outs, 0)
    weight_grad(mixed, order[...], above[...], outs, 3 * rolled.shape[1])


def merge_backward(
    b0, b1, b2, b3, merged, cot, two, sel_back, gain3, gain, weight, edges,
    out_o, d_two_o, d_rows_o, gm_o, g3_o, e0, e1, e2,
):
    back = pick(sel_back[...], joined((b0, b1, b2, b3)))
    width = merged.shape[1]
    base = merged[...].astype(F32)
    out = base + back[:, :width].astype(F32)
    rows, cols = out_o.shape[:2]
    pad = out.shape[0] // rows
    for r in range(rows):
        out_o[r] = out[r * pad : r * pad + cols].astype(BF)
    d_normed = back[:, width:].astype(F32)
    d_merged, g3 = norm_back(base, gain3[...], d_normed)
    g3_o[...] = g3
    d_rows = (cot[...].astype(F32) + d_merged.astype(F32)).astype(BF)
    d_rows_o[...] = d_rows
    d_norm = mm_nt(d_rows, weight[...]).astype(BF).astype(F32)
    d_wide, gm = norm_back(two[...].astype(F32), gain[...], d_norm)
    gm_o[...] = gm
    quarter = d_wide.shape[1] // 4
    d_two = jnp.concatenate([d_wide[:, k * quarter : (k + 1) * quarter] for k in range(4)], axis=0)
    d_two_o[...] = d_two
    put_edges(d_two, edges[...], (e0, e1, e2))


def merge_grads(norm, d_rows, order, send_o, keep_o):
    weight_grad(norm, order[...], d_rows[...], (send_o, keep_o), 0, halves=2)


def two_backward(
    d0, d1, d2, d3, mixed, packed, rolled, qkv, proj, gain, sel, bias, edges, order, gm, g3,
    wins_o, send_o, keep_o, e0, e1, e2, d_packed, d_mixed,
):
    above = pick(sel[...], joined((d0, d1, d2, d3)))
    width = above.shape[1]
    d_mixed[...] = mm_nt(above, proj[...]).astype(BF)

    def step(g, carry):
        rows = pl.ds(pl.multiple_of(g * PAIR, PAIR), PAIR)
        mask = tiled_bias(bias[g])
        for t in range(width // TILE):
            q, k, v = thirds(packed, rows, width, t)
            tall, share = soft(q, k, mask)
            given = stacked(d_mixed[rows, t * TILE : (t + 1) * TILE])
            put_thirds(d_packed, rows, width, t, head_grads(tall, share, given, k, v))
        return carry

    lax.fori_loop(0, packed.shape[0] // PAIR, step, 0)
    d_rolled = mm_nt(d_packed[...], qkv[...]).astype(BF)
    wins_o[...] = d_rolled
    put_edges(d_rolled, edges[...], (e0, e1, e2))
    outs = (send_o, keep_o)
    weight_grad(rolled, order[...], d_packed[...], outs, 0)
    weight_grad(mixed, order[...], above, outs, 3 * width)
    g2 = jnp.sum(d_rolled.astype(F32) * rolled[...].astype(F32), axis=0, keepdims=True) / gain[...]
    blank = jnp.zeros((1, width), F32)
    second = jnp.concatenate([g3[...], g2, blank], axis=1)
    line = lax.broadcasted_iota(jnp.int32, (16, 4 * width), 0)
    gains = jnp.where(line == 0, gm[...], jnp.where(line == 1, second, 0.0)).astype(BF)
    for out in outs:
        xs, rows = out.shape[:2]
        for x in range(xs):
            out[x, rows - 16 :, :] = gains


def tokens_backward(w0, w1, w2, w3, tokens, d_two, gain, sel_back, sel_out, out_o):
    d_normed = pick(sel_back[...], joined((w0, w1, w2, w3)))
    d_norm, _ = norm_back(tokens[...].astype(F32), gain[...], d_normed.astype(F32))
    total = (d_two[...].astype(F32) + d_norm.astype(F32)).astype(BF)
    laid = pick(sel_out[...], total)
    rows, cols = out_o.shape[:2]
    pad = laid.shape[0] // rows
    for r in range(rows):
        out_o[r] = laid[r * pad : r * pad + cols]


def pair_sum(keep, got, *outs):
    for x, out in enumerate(outs):
        out[...] = (keep[x].astype(F32) + got[x].astype(F32)).astype(BF)


def added(parts):
    parts = [p[...].astype(F32) for p in parts]
    while len(parts) > 1:
        half = len(parts) // 2
        parts = [parts[j] + parts[j + half] for j in range(half)]
    return parts[0]


def make_line_sum(rows, near, sub):
    far = rows // near
    size = far * sub

    def line_sum(where, *refs):
        held, outs = refs[: len(refs) - near], refs[len(refs) - near :]
        count = len(held) // 3
        p = lines(rows * sub)
        j, a, k = div(p, size), div(mod(p, size), sub), mod(p, sub)
        row = a * near + mod(mod(where[0], near) + j, near)
        at = 0
        for b in range(3):
            total = added(held[b * count : (b + 1) * count]).astype(BF)
            wanted = row * sub + k
            if b == 2:
                share = total.shape[0] - 16
                part = share // rows
                wanted = jnp.where(k < part, row * part + k, share + k - part)
            laid = pick(one_hot(wanted, total.shape[0]), total)
            for j, out in enumerate(outs):
                out[:, at : at + laid.shape[1]] = laid[j * size : (j + 1) * size]
            at += laid.shape[1]

    def near_sum(where, *refs):
        held, outs = refs[:near], refs[near:]
        total = added(held).astype(BF)
        p = lines(size)
        own = div(where[0], near)
        wanted = mod(own + div(p, sub), far) * sub + mod(p, sub)
        laid = mm(one_hot(wanted, size), total)
        for j, out in enumerate(outs):
            out[...] = laid[j * sub : (j + 1) * sub].astype(BF)

    return line_sum, near_sum


def flat_lines(value, lo, width):
    parts = []
    for r in range(value.shape[0]):
        for at in range(lo, lo + width, TILE):
            parts.append(value[r : r + 1, at : at + TILE])
    return parts


def make_finish(wide, narrow, sub2, far):
    def finish(*refs):
        held, (gains_o, qkv2_o, proj2_o, merge_o, qkv3_o, proj3_o) = refs[:far], refs[far:]
        total = added(held)
        at = 6 * wide
        late = total[:sub2]
        extra = total[sub2 : sub2 + 2]
        first, second = extra[:1], extra[1:]
        gains = (
            flat_lines(second, at + wide, narrow)
            + flat_lines(first, at, 4 * narrow)
            + flat_lines(second, at, wide)
        )
        for out, parts in (
            (gains_o, gains),
            (qkv2_o, flat_lines(late, at, 3 * narrow)),
            (proj2_o, flat_lines(late, at + 3 * narrow, narrow)),
            (merge_o, flat_lines(total, 4 * wide, wide) + flat_lines(total, 5 * wide, wide)),
            (qkv3_o, flat_lines(total, 0, 3 * wide)),
            (proj3_o, flat_lines(total, 3 * wide, wide)),
        ):
            out[...] = jnp.concatenate(parts, axis=0).astype(out.dtype)

    return finish


def call(body, outs, args, flops, scratch=(), scalars=0):
    smem, vmem = (pl.BlockSpec(memory_space=m) for m in (pltpu.SMEM, pltpu.VMEM))
    return pl.pallas_call(
        body,
        in_specs=[smem] * scalars + [vmem] * (len(args) - scalars),
        out_shape=[jax.ShapeDtypeStruct(shape, kind) for shape, kind in outs],
        scratch_shapes=[pltpu.VMEM(shape, kind) for shape, kind in scratch],
        cost_estimate=pl.CostEstimate(flops=flops, transcendentals=0, bytes_accessed=4 << 20),
        compiler_params=pltpu.CompilerParams(vmem_limit_bytes=8 << 20),
    )(*args)


def moved(value, axis, by):
    count = lax.axis_size(axis)
    return lax.ppermute(value, axis, [(i, (i + by) % count) for i in range(count)])


def moved_across(value, by):
    rows, cols = lax.axis_size("rows"), lax.axis_size(COLS)
    pairs = [
        (i * cols + j, ((i + by) % rows) * cols + (j + by) % cols)
        for i in range(rows)
        for j in range(cols)
    ]
    return lax.ppermute(value, ROWS_COLS, pairs)


def to_neighbours(pieces, by):
    rows, cols, corner = pieces
    return moved_across(corner, by), moved(rows, "rows", by), moved(cols, COLS, by)


def exchanged(pieces, by):
    corner, rows, cols = to_neighbours(pieces, by)
    return rows, cols, corner


def core_sum(send, keep):
    got = moved(send, "cols_1", 1)
    shape = (keep.shape[1:], BF)
    return call(pair_sum, [shape] * keep.shape[0], (keep, got), 1 << 26)


def line_parts(blocks):
    return [blocks[0]] + [moved(blocks[j], "cols_0", j) for j in range(1, len(blocks))]


def moved_near(value, by, near):
    count = lax.axis_size("rows")
    pairs = [(i, i - i % near + (i % near + by) % near) for i in range(count)]
    return lax.ppermute(value, "rows", pairs)


def on_device(
    tokens,
    cotangent,
    shift_offsets,
    norm2_gain,
    qkv2,
    proj2,
    merge_gain,
    merge_weight,
    norm3_gain,
    qkv3,
    proj3,
):
    tile_rows, tile_cols, narrow = tokens.shape
    three_rows, three_cols, wide = cotangent.shape
    ranks = tuple(lax.axis_size(a) for a in ROWS_COLS)
    rows, xs, cores = ranks
    pad, pad3 = up16(tile_cols), up16(three_cols)
    size3 = three_rows * pad3
    n2 = (tile_rows // WIN) * (tile_cols // WIN) * SLOT
    n3 = (three_rows // WIN) * (three_cols // WIN) * SLOT
    n4 = 4 * size3
    er, ec, ex = up16(EDGE * tile_cols), up16(tile_rows * EDGE), up16(EDGE * EDGE)
    hr, tr, hc = EDGE * pad3, up16(EDGE * three_cols), up16(three_rows * EDGE)
    gain2, gain_m, gain3 = norm2_gain[None], merge_gain[None], norm3_gain[None]

    tokens_p, *pieces = call(
        input_edges,
        [
            ((tile_rows * pad, narrow), BF),
            ((EDGE * pad, narrow), BF),
            ((ec, narrow), BF),
            ((ex, narrow), BF),
        ],
        (tokens,),
        1 << 28,
    )
    token_pieces = exchanged(pieces, -1)
    cot_p, *pieces = call(
        input_edges,
        [((size3, wide), BF), ((hr, wide), BF), ((hc, wide), BF), ((ex, wide), BF)],
        (cotangent,),
        1 << 28,
    )
    cot_pieces = exchanged(pieces, -1)
    where = jnp.stack([lax.axis_index(a) for a in ROWS_COLS]).astype(jnp.int32)
    early, early_shapes, late, late_shapes = make_tables(
        (tile_rows, tile_cols), (three_rows, three_cols), ranks, (narrow, wide, 4 * narrow)
    )
    scalars = (shift_offsets, where)
    sel_a, tail2, sel_tokens, sel_b, head3, bias2 = call(
        early, early_shapes, scalars, 1 << 28, scalars=2
    )
    sel3, tail3, sel3b, head2, sel_e, sel_out, order2, order3, order_m, bias3 = call(
        late, late_shapes, scalars, 1 << 28, scalars=2
    )

    rolled, packed, mixed, wins, *edges = call(
        two_forward,
        [
            ((n2, narrow), BF),
            ((n2, 3 * narrow), BF),
            ((n2, narrow), BF),
            ((n2, narrow), BF),
            ((er, narrow), BF),
            ((ec, narrow), BF),
            ((ex, narrow), BF),
        ],
        (tokens_p, *token_pieces, gain2, qkv2, proj2, sel_a, bias2, tail2),
        1 << 30,
    )
    back = exchanged(edges, 1)
    two, tokens_q, merged_norm, merged, normed3, *edges = call(
        merge_forward,
        [
            ((size3, 4 * narrow), BF),
            ((n4, narrow), BF),
            ((size3, 4 * narrow), BF),
            ((size3, wide), BF),
            ((size3, wide), BF),
            ((hr, wide), BF),
            ((hc, wide), BF),
            ((ex, wide), BF),
        ],
        (tokens_p, wins, *back, sel_tokens, sel_b, gain_m, merge_weight, gain3, head3),
        1 << 30,
    )
    ahead = exchanged(edges, -1)
    both, rolled3, above3, mixed3, d_packed3, *edges = call(
        three_both,
        [
            ((n3, 2 * wide), BF),
            ((n3, wide), BF),
            ((n3, wide), BF),
            ((n3, wide), BF),
            ((n3, 3 * wide), BF),
            ((tr, 2 * wide), BF),
            ((hc, 2 * wide), BF),
            ((ex, 2 * wide), BF),
        ],
        (normed3, *ahead, cot_p, *cot_pieces, qkv3, proj3, sel3, bias3, tail3),
        1 << 30,
        scratch=[((n3, 3 * wide), BF), ((n3, wide), BF)],
    )
    back = exchanged(edges, 1)
    share3 = wide // (xs * cores)
    send, keep = call(
        three_grads,
        [((xs, share3, 4 * wide), BF)] * 2,
        (rolled3, above3, mixed3, d_packed3, order3),
        1 << 30,
    )
    sum_a = core_sum(send, keep)
    merged_out, d_two, d_rows, grad_m, grad_3, *edges = call(
        merge_backward,
        [
            ((three_rows, three_cols, wide), BF),
            ((n4, narrow), BF),
            ((size3, wide), BF),
            ((1, 4 * narrow), F32),
            ((1, wide), F32),
            ((er, narrow), BF),
            ((ec, narrow), BF),
            ((ex, narrow), BF),
        ],
        (both, *back, merged, cot_p, two, sel3b, gain3, gain_m, merge_weight, head2),
        1 << 30,
    )
    ahead = exchanged(edges, -1)
    send, keep = call(
        merge_grads, [((xs, share3, 2 * wide), BF)] * 2, (merged_norm, d_rows, order_m), 1 << 30
    )
    sum_b = core_sum(send, keep)
    share2 = narrow // (xs * cores)
    wins, send, keep, *edges = call(
        two_backward,
        [
            ((n2, narrow), BF),
            ((xs, share2 + 16, 4 * narrow), BF),
            ((xs, share2 + 16, 4 * narrow), BF),
            ((er, narrow), BF),
            ((ec, narrow), BF),
            ((ex, narrow), BF),
        ],
        (
            d_two, *ahead, mixed, packed, rolled, qkv2, proj2, gain2, sel_e, bias2, tail2,
            order2, grad_m, grad_3,
        ),
        1 << 30,
        scratch=[((n2, 3 * narrow), BF), ((n2, narrow), BF)],
    )
    back = exchanged(edges, 1)
    sum_c = core_sum(send, keep)
    (tokens_grad,) = call(
        tokens_backward,
        [((tile_rows, tile_cols, narrow), BF)],
        (wins, *back, tokens_q, d_two, gain2, sel_b, sel_out),
        1 << 30,
    )

    sub = wide // (rows * xs * cores)
    sub2 = narrow // (rows * xs * cores)
    far = rows // NEAR
    lanes = 6 * wide + 4 * narrow
    sum_lines, sum_near = make_line_sum(rows, NEAR, sub)
    held = line_parts(sum_a) + line_parts(sum_b) + line_parts(sum_c)
    parts = call(sum_lines, [((far * sub, lanes), BF)] * NEAR, (where, *held), 1 << 26, scalars=1)
    held = [parts[0]] + [moved_near(parts[j], j, NEAR) for j in range(1, NEAR)]
    parts = call(sum_near, [((sub, lanes), BF)] * far, (where, *held), 1 << 26, scalars=1)
    held = [parts[0]] + [moved(parts[j], "rows", j * NEAR) for j in range(1, far)]
    sizes = (
        (narrow + 4 * narrow + wide, F32),
        (sub2 * 3 * narrow, BF),
        (sub2 * narrow, BF),
        (2 * sub * wide, BF),
        (sub * 3 * wide, BF),
        (sub * wide, BF),
    )
    grads = call(
        make_finish(wide, narrow, sub2, far),
        [((size // TILE, TILE), kind) for size, kind in sizes],
        held,
        1 << 26,
    )
    return (merged_out, tokens_grad, *(g.reshape(-1) for g in grads))


def solution(mesh):
    cores = 2
    split = Mesh(
        mesh.devices.reshape(
            mesh.shape["groups"], mesh.shape["rows"], mesh.shape["cols"] // cores, cores
        ),
        ("groups", "rows", "cols_0", "cols_1"),
    )
    tiles = P(("groups", "rows"), COLS, None)
    flat = P(GROUPS_ROWS_COLS)


    return jax.shard_map(
        on_device,
        mesh=split,
        in_specs=(tiles, tiles) + (P(),) * 9,
        out_specs=(tiles, tiles, P("groups"), flat, flat, flat, flat, flat),
        check_vma=False,
    )
```

```python
import functools

import jax
import jax.numpy as jnp
from jax import lax
from jax.experimental import pallas as pl
from jax.experimental.pallas import tpu as pltpu
from jax.sharding import Mesh
from jax.sharding import PartitionSpec as P


WIN = 7
AREA = WIN * WIN
SLOT = 64
PAIR = 2 * SLOT
TILE = 128
HEAD = 32
EDGE = WIN - 1
NEAR = 4
COLS = ("cols_0", "cols_1")
ROWS_COLS = ("rows", "cols_0", "cols_1")
GROUPS_ROWS_COLS = ("groups", "rows", "cols_0", "cols_1")

EPSILON = 1e-05
MASKED = -100.0
APART = -1e30
BF = jnp.bfloat16
F32 = jnp.float32


def up16(count):
    return -(-count // 16) * 16


def mm(a, b):
    return lax.dot_general(a, b, (((1,), (0,)), ((), ())), preferred_element_type=F32)


def mm_nt(a, b):
    return lax.dot_general(a, b, (((1,), (1,)), ((), ())), preferred_element_type=F32)


def mm_tn(a, b):
    return lax.dot_general(a, b, (((0,), (0,)), ((), ())), preferred_element_type=F32)


def pick(selection, source):
    return mm(selection, source).astype(BF)


def norm_parts(values):
    centred = values - jnp.mean(values, axis=-1, keepdims=True)
    spread = jnp.mean(centred * centred, axis=-1, keepdims=True)
    scale = lax.rsqrt(spread + EPSILON)
    return centred * scale, scale


def normed(values, gain):
    return (norm_parts(values)[0] * gain).astype(BF)


def norm_back(values, gain, upstream):
    unit, scale = norm_parts(values)
    inner = upstream * gain
    along = jnp.mean(inner * unit, axis=-1, keepdims=True)
    grad = scale * (inner - jnp.mean(inner, axis=-1, keepdims=True) - unit * along)
    return grad.astype(BF), jnp.sum(upstream * unit, axis=0, keepdims=True)


def lane_head(shape):
    return lax.broadcasted_iota(jnp.int32, shape, 1) // HEAD


def stacked(block):
    heads = lane_head((1, TILE))
    parts = [block * (heads == h).astype(F32).astype(BF) for h in range(TILE // HEAD)]
    return jnp.concatenate(parts, axis=0)


def unstacked(tall):
    heads = lane_head((PAIR, TILE))
    out = tall[:PAIR]
    for h in range(1, TILE // HEAD):
        out = jnp.where(heads == h, tall[h * PAIR : (h + 1) * PAIR], out)
    return out


def soft(queries, keys, bias):
    tall = stacked(queries)
    raised = jnp.exp(mm_nt(tall, keys) * HEAD ** (-0.5) + bias)
    return tall, raised / jnp.sum(raised, axis=-1, keepdims=True)


def tiled_bias(bias):
    return jnp.concatenate([bias] * (TILE // HEAD), axis=0)


def tile_at(start):
    if isinstance(start, int):
        return slice(start, start + TILE)
    return pl.ds(pl.multiple_of(start, TILE), TILE)


def thirds(packed, rows, width, t):
    return (packed[rows, tile_at(p * width + t * TILE)] for p in range(3))


def head_grads(tall, share, above, k, v):
    d_share = mm_nt(above, v).astype(BF).astype(F32)
    along = jnp.sum(d_share * share, axis=-1, keepdims=True)
    d_scores = (share * (d_share - along) * HEAD ** (-0.5)).astype(BF)
    return (
        unstacked(mm(d_scores, k)),
        mm_tn(d_scores, tall),
        mm_tn(share.astype(BF), above),
    )


def put_thirds(out, rows, width, t, grads):
    for p, grad in enumerate(grads):
        out[rows, tile_at(p * width + t * TILE)] = grad.astype(BF)


def put_pieces(grad, outs, block, lanes, halves=1):
    cores, xs = len(outs), outs[0].shape[0]
    size = grad.shape[0] // (cores * xs * halves)
    width = grad.shape[1]
    rows = pl.ds(pl.multiple_of(block * size, size), size)
    for h in range(halves):
        for c in range(cores):
            for x in range(xs):
                at = ((h * cores + c) * xs + x) * size
                lo = lanes + h * width
                outs[c][x, rows, lo : lo + width] = grad[at : at + size].astype(BF)


def weight_grad(acts, order, upstream, outs, lanes, halves=1):
    side = order.shape[0]

    def step(block, carry):
        cols = pl.ds(pl.multiple_of(block * side, side), side)
        moved_cols = pick_cols(acts[:, cols], order)
        put_pieces(mm_tn(moved_cols, upstream), outs, block, lanes, halves)
        return carry

    lax.fori_loop(0, acts.shape[1] // side, step, 0)


def pick_cols(acts, order):
    return mm(acts, order).astype(BF)


def put_edges(values, edges, outs):
    sent = pick(edges, values)
    at = 0
    for out in outs:
        out[...] = sent[at : at + out.shape[0]]
        at += out.shape[0]


def joined(refs):
    return jnp.concatenate([r[...] for r in refs], axis=0)


def div(value, by):
    return (value * (-(-65536 // by))) >> 16


def mod(value, by):
    return value - div(value, by) * by


def lines(count, at=0):
    return lax.broadcasted_iota(jnp.int32, (count, 1), 0) + at


def one_hot(wanted, width):
    return (wanted == lax.broadcasted_iota(jnp.int32, (wanted.shape[0], width), 1)).astype(F32).astype(BF)


def strip(p, height, breadth, place, row0=0, col0=0):
    r, c = div(p, breadth), mod(p, breadth)
    return jnp.where(p < height * breadth, place(r + row0, c + col0), -1)


def input_edges(tokens, cot, tokens_o, cot_o, rows_o, cols_o, corner_o):
    narrow = tokens.shape[2]
    at = [0, 0, 0]
    for source, laid in ((tokens, tokens_o), (cot, cot_o)):
        rows, cols, width = source.shape
        pad = laid.shape[0] // rows
        blank = jnp.zeros((pad - cols, width), F32)
        parts = []
        for r in range(rows):
            parts += [source[r].astype(F32), blank]
        whole = jnp.concatenate(parts, axis=0).astype(BF)
        laid[...] = whole

        def place(r, c, pad=pad):
            return r * pad + c

        def edge(height, whole=whole, place=place):
            wanted = strip(lines(up16(height * EDGE)), height, EDGE, place)
            return pick(one_hot(wanted, whole.shape[0]), whole)

        edges = (whole[: EDGE * pad], edge(rows), edge(EDGE))
        for k, (out, value) in enumerate(zip((rows_o, cols_o, corner_o), edges)):
            for lo in range(0, width, narrow):
                out[at[k] : at[k] + value.shape[0], :] = value[:, lo : lo + narrow]
                at[k] += value.shape[0]


def cotangent_part(piece, first, wide):
    narrow = piece.shape[1]
    size = (piece.shape[0] - first) // (wide // narrow)
    return jnp.concatenate(
        [piece[first + k * size : first + (k + 1) * size] for k in range(wide // narrow)], axis=1
    )


def make_tables(tile, tile3, ranks, depths):
    tile_rows, tile_cols = tile
    three_rows, three_cols = tile3
    pad, pad3 = up16(tile_cols), up16(three_cols)
    size3 = three_rows * pad3
    line2, line3 = tile_cols // WIN, three_cols // WIN
    count2 = line2 * (tile_rows // WIN)
    count3 = line3 * (three_rows // WIN)
    er, ec, ex = up16(EDGE * tile_cols), up16(tile_rows * EDGE), up16(EDGE * EDGE)
    tr, hc = up16(EDGE * three_cols), up16(three_rows * EDGE)
    hr = EDGE * pad3
    main_n, rows_n = tile_rows * pad, EDGE * pad
    n2, n3, n4 = count2 * SLOT, count3 * SLOT, 4 * size3
    rows, xs, cores = ranks

    def window_line(p, line):
        w, t = div(p, SLOT), mod(p, SLOT)
        row = div(w, line) * WIN + div(t, WIN)
        col = mod(w, line) * WIN + mod(t, WIN)
        return t < AREA, row, col

    def window_place(row, col, line):
        w = div(row, WIN) * line + div(col, WIN)
        return w * SLOT + mod(row, WIN) * WIN + mod(col, WIN)

    def in_windows2(r, c):
        return window_place(r, c, line2)

    def in_windows3(r, c):
        return window_place(r, c, line3)

    def in_planes(r, c):
        return (mod(c, 2) * 2 + mod(r, 2)) * size3 + div(r, 2) * pad3 + div(c, 2)

    def pick4(low, right, main, strip_rows, strip_cols, corner):
        return jnp.where(low, jnp.where(right, corner, strip_rows), jnp.where(right, strip_cols, main))

    def ahead(p, line, extent, shifts, place, main, breadth, strip_rows, strip_cols):
        valid, row, col = window_line(p, line)
        r, c = row + shifts[0], col + shifts[1]
        a, b = r - extent[0], c - extent[1]
        at = pick4(
            a >= 0,
            b >= 0,
            place(r, c),
            main + a * breadth + c,
            main + strip_rows + r * EDGE + b,
            main + strip_rows + strip_cols + a * EDGE + b,
        )
        return jnp.where(valid, at, -1)

    def behind(real, r, c, place, main, extent, strip_rows, strip_cols):
        at = pick4(
            r < 0,
            c < 0,
            place(jnp.maximum(r, 0), jnp.maximum(c, 0)),
            main + (r + EDGE) * extent[1] + c,
            main + strip_rows + r * EDGE + c + EDGE,
            main + strip_rows + strip_cols + (r + EDGE) * EDGE + c + EDGE,
        )
        return jnp.where(real, at, -1)

    def edges(p, place, extent, first, sizes):
        h = strip(p, EDGE, extent[1], place, first[0], 0)
        v = strip(p - sizes[0], extent[0], EDGE, place, 0, first[1])
        x = strip(p - sizes[0] - sizes[1], EDGE, EDGE, place, first[0], first[1])
        return jnp.where(p < sizes[0], h, jnp.where(p < sizes[0] + sizes[1], v, x))

    def grid_of(q):
        k, m = div(q, size3), mod(q, size3)
        a, b = div(m, pad3), mod(m, pad3)
        return b < three_cols, 2 * a + mod(k, 2), 2 * b + div(k, 2)

    def fill(out, wanted_of, block):
        def step(i, carry):
            at = pl.multiple_of(i * block, block)
            out[pl.ds(at, block), :] = one_hot(wanted_of(lines(block, at)), out.shape[1])
            return carry

        lax.fori_loop(0, out.shape[0] // block, step, 0)

    def in_pad(r, c):
        return r * pad + c

    def in_pad3(r, c):
        return r * pad3 + c

    def label(at, extent, shift):
        return jnp.where(at < extent - WIN, 0, jnp.where(at < extent - shift, 1, 2))

    def bias(where, first, line, extent, shifts):
        row_rank, x_rank, c_rank = (where[i] for i in range(3))
        col_rank = x_rank * cores + c_rank

        def marks(p):
            valid, row, col = window_line(p, line)
            r = label(row + row_rank * extent[0], extent[0] * rows, shifts[0])
            c = label(col + col_rank * extent[1], extent[1] * xs * cores, shifts[1])
            near = div(p, SLOT) * 2 + jnp.where(valid, 1, 0)
            return near, jnp.where(valid, r * 3 + c, -1)

        near_p, mark_p = marks(lines(PAIR, first))
        near_q, mark_q = marks(lax.broadcasted_iota(jnp.int32, (1, PAIR), 1) + first)
        same = jnp.where(mark_p == mark_q, 0.0, MASKED)
        return jnp.where(near_p == near_q, same, APART).astype(F32)

    def early(offsets, where, sel_a, tail2, sel_tokens, sel_b, head3, bias2):
        s0, s1 = offsets[0], offsets[1]
        fill(
            sel_a,
            lambda p: ahead(p, line2, tile, (s0, s1), in_pad, main_n, pad, rows_n, ec),
            32,
        )
        fill(
            tail2,
            lambda p: edges(p, in_windows2, tile, (tile_rows - EDGE, tile_cols - EDGE), (er, ec)),
            32,
        )

        def from_grid(q):
            real, r, c = grid_of(q)
            return jnp.where(real, in_pad(r, c), -1)

        fill(sel_tokens, from_grid, 32)

        def back2(q):
            real, r, c = grid_of(q)
            return behind(real, r - s0, c - s1, in_windows2, n2, tile, er, ec)

        fill(sel_b, back2, 32)

        def head_of_three(p):
            v = strip(p - hr, three_rows, EDGE, in_pad3)
            x = strip(p - hr - hc, EDGE, EDGE, in_pad3)
            return jnp.where(p < hr, p, jnp.where(p < hr + hc, v, x))

        fill(head3, head_of_three, 16)
        for g in range(bias2.shape[0]):
            bias2[g] = bias(where, g * PAIR, line2, tile, (s0, s1))

    def late(
        offsets, where, sel3, tail3, sel3b, head2, sel_e, sel_out, order2, order3, order_m, bias3
    ):
        s0, s1, s2, s3 = (offsets[i] for i in range(4))
        x_rank, c_rank = where[1], where[2]
        fill(
            sel3,
            lambda p: ahead(p, line3, tile3, (s2, s3), in_pad3, size3, pad3, hr, hc),
            32,
        )
        fill(
            tail3,
            lambda p: edges(
                p, in_windows3, tile3, (three_rows - EDGE, three_cols - EDGE), (tr, hc)
            ),
            16,
        )

        def back3(m):
            a, b = div(m, pad3), mod(m, pad3)
            return behind(b < three_cols, a - s2, b - s3, in_windows3, n3, tile3, tr, hc)

        fill(sel3b, back3, 16)
        fill(head2, lambda p: edges(p, in_planes, tile, (0, 0), (er, ec)), 32)
        fill(
            sel_e,
            lambda p: ahead(p, line2, tile, (s0, s1), in_planes, n4, tile_cols, er, ec),
            32,
        )

        def to_grid(g):
            return jnp.where(mod(g, pad) < tile_cols, in_planes(div(g, pad), mod(g, pad)), -1)

        fill(sel_out, to_grid, 32)

        for out, depth, halves in ((order2, depths[0], 1), (order3, depths[1], 1), (order_m, depths[2], 2)):
            side = out.shape[0]
            per_row = depth // rows
            near = side // per_row
            sub = depth // (rows * xs * cores)
            part = sub // halves
            at = lax.broadcasted_iota(jnp.int32, (1, side), 1)
            r = mod(div(at, part), near)
            x = mod(div(at, part * near) + x_rank, xs)
            c = mod(div(at, part * near * xs) + 1 + c_rank, cores)
            h = div(at, part * near * xs * cores)
            source = r * per_row + (x * cores + c) * sub + h * part + mod(at, part)
            lanes = lax.broadcasted_iota(jnp.int32, (side, side), 0)
            out[...] = (lanes == source).astype(F32).astype(BF)

        bias3[...] = bias(where, 0, line3, tile3, (s2, s3))

    early_shapes = [
        ((n2, main_n + rows_n + ec + ex), BF),
        ((er + ec + ex, n2), BF),
        ((n4, main_n), BF),
        ((n4, n2 + er + ec + ex), BF),
        ((hr + hc + ex, size3), BF),
        ((n2 // PAIR, PAIR, PAIR), F32),
    ]
    late_shapes = [
        ((n3, size3 + hr + hc + ex), BF),
        ((tr + hc + ex, n3), BF),
        ((size3, n3 + tr + hc + ex), BF),
        ((er + ec + ex, n4), BF),
        ((n2, n4 + er + ec + ex), BF),
        ((main_n, n4), BF),
        ((256, 256), BF),
        ((256, 256), BF),
        ((256, 256), BF),
        ((PAIR, PAIR), F32),
    ]
    return early, early_shapes, late, late_shapes


def two_forward(
    sizes, t0, t1, t2, t3, gain, qkv, proj, sel, bias, edges, rolled_o, packed_o, mixed_o, wins_o, e0, e1, e2
):
    held = [t0[...]] + [t[:size] for t, size in zip((t1, t2, t3), sizes)]
    tokens = pick(sel[...], jnp.concatenate(held, axis=0))
    rolled = normed(tokens.astype(F32), gain[...])
    rolled_o[...] = rolled
    packed_o[...] = mm(rolled, qkv[...]).astype(BF)
    width = rolled.shape[1]

    def step(g, carry):
        for pair in (2 * g, 2 * g + 1):
            rows = slice(pair * PAIR, (pair + 1) * PAIR)
            mask = tiled_bias(bias[pair])
            for t in range(width // TILE):
                q, k, v = thirds(packed_o, rows, width, t)
                share = soft(q, k, mask)[1].astype(BF)
                mixed_o[rows, tile_at(t * TILE)] = unstacked(mm(share, v)).astype(BF)
        return carry

    for g in range(packed_o.shape[0] // (2 * PAIR)):
        step(g, 0)
    projected = mm(mixed_o[...], proj[...]).astype(BF)
    wins_o[...] = projected
    put_edges(projected, edges[...], (e0, e1, e2))


def merge_forward(
    tokens, w0, w1, w2, w3, sel_tokens, sel_back, gain, weight, gain3, edges,
    two_o, tokens_o, norm_o, merged_o, normed_o, e0, e1, e2,
):
    laid = pick(sel_tokens[...], tokens[...])
    back = pick(sel_back[...], joined((w0, w1, w2, w3)))
    two = (laid.astype(F32) + back.astype(F32)).astype(BF)
    tokens_o[...] = laid
    size = two.shape[0] // 4
    wide = jnp.concatenate([two[k * size : (k + 1) * size] for k in range(4)], axis=1)
    two_o[...] = wide
    merged_norm = normed(wide.astype(F32), gain[...])
    norm_o[...] = merged_norm
    merged = mm(merged_norm, weight[...]).astype(BF)
    merged_o[...] = merged
    three = normed(merged.astype(F32), gain3[...])
    normed_o[...] = three
    put_edges(three, edges[...], (e0, e1, e2))


def three_both(
    sizes, n0, n1, n2, n3, c0, c1, c2, c3, qkv, proj, sel, bias, edges,
    both_o, rolled_o, above_o, mixed, d_packed, e0, e1, e2, packed, d_mixed,
):
    rolled = pick(sel[...], joined((n0, n1, n2, n3)))
    cots = [c0[...]] + [
        cotangent_part(c[...], size, c0.shape[1]) for c, size in zip((c1, c2, c3), sizes)
    ]
    above = pick(sel[...], jnp.concatenate(cots, axis=0))
    rolled_o[...] = rolled
    above_o[...] = above
    width = rolled.shape[1]
    packed[...] = mm(rolled, qkv[...]).astype(BF)
    d_mixed[...] = mm_nt(above, proj[...]).astype(BF)
    mask = tiled_bias(bias[...])
    rows = slice(0, PAIR)

    def step(i, carry):
        for t in (2 * i, 2 * i + 1):
            lanes = tile_at(t * TILE)
            q, k, v = thirds(packed, rows, width, t)
            tall, share = soft(q, k, mask)
            mixed[rows, lanes] = unstacked(mm(share.astype(BF), v)).astype(BF)
            given = stacked(d_mixed[rows, lanes])
            put_thirds(d_packed, rows, width, t, head_grads(tall, share, given, k, v))
        return carry

    for i in range(width // (2 * TILE)):
        step(i, 0)
    projected = mm(mixed[...], proj[...]).astype(BF)
    d_rolled = mm_nt(d_packed[...], qkv[...]).astype(BF)
    both = jnp.concatenate([projected, d_rolled], axis=1)
    both_o[...] = both
    put_edges(both, edges[...], (e0, e1, e2))


def three_grads(rolled, above, mixed, d_packed, order, send_o, keep_o):
    outs = (send_o, keep_o)
    weight_grad(rolled, order[...], d_packed[...], outs, 0)
    weight_grad(mixed, order[...], above[...], outs, 3 * rolled.shape[1])


def merge_backward(
    b0, b1, b2, b3, merged, cot, two, sel_back, gain3, gain, weight, edges,
    out_o, d_two_o, d_rows_o, gm_o, g3_o, e0, e1, e2,
):
    back = pick(sel_back[...], joined((b0, b1, b2, b3)))
    width = merged.shape[1]
    base = merged[...].astype(F32)
    out = base + back[:, :width].astype(F32)
    rows, cols = out_o.shape[:2]
    pad = out.shape[0] // rows
    for r in range(rows):
        out_o[r] = out[r * pad : r * pad + cols].astype(BF)
    d_normed = back[:, width:].astype(F32)
    d_merged, g3 = norm_back(base, gain3[...], d_normed)
    g3_o[...] = g3
    d_rows = (cot[...].astype(F32) + d_merged.astype(F32)).astype(BF)
    d_rows_o[...] = d_rows
    d_norm = mm_nt(d_rows, weight[...]).astype(BF).astype(F32)
    d_wide, gm = norm_back(two[...].astype(F32), gain[...], d_norm)
    gm_o[...] = gm
    quarter = d_wide.shape[1] // 4
    d_two = jnp.concatenate([d_wide[:, k * quarter : (k + 1) * quarter] for k in range(4)], axis=0)
    d_two_o[...] = d_two
    put_edges(d_two, edges[...], (e0, e1, e2))


def merge_grads(norm, d_rows, order, send_o, keep_o):
    weight_grad(norm, order[...], d_rows[...], (send_o, keep_o), 0, halves=2)


def two_backward(
    d0, d1, d2, d3, mixed, packed, rolled, qkv, proj, gain, sel, bias, edges, order, gm, g3,
    wins_o, send_o, keep_o, e0, e1, e2, d_packed, d_mixed,
):
    above = pick(sel[...], joined((d0, d1, d2, d3)))
    width = above.shape[1]
    d_mixed[...] = mm_nt(above, proj[...]).astype(BF)

    def step(g, carry):
        rows = pl.ds(pl.multiple_of(g * PAIR, PAIR), PAIR)
        mask = tiled_bias(bias[g])
        for t in range(width // TILE):
            q, k, v = thirds(packed, rows, width, t)
            tall, share = soft(q, k, mask)
            given = stacked(d_mixed[rows, t * TILE : (t + 1) * TILE])
            put_thirds(d_packed, rows, width, t, head_grads(tall, share, given, k, v))
        return carry

    lax.fori_loop(0, packed.shape[0] // PAIR, step, 0)
    d_rolled = mm_nt(d_packed[...], qkv[...]).astype(BF)
    wins_o[...] = d_rolled
    put_edges(d_rolled, edges[...], (e0, e1, e2))
    outs = (send_o, keep_o)
    weight_grad(rolled, order[...], d_packed[...], outs, 0)
    weight_grad(mixed, order[...], above, outs, 3 * width)
    g2 = jnp.sum(d_rolled.astype(F32) * rolled[...].astype(F32), axis=0, keepdims=True) / gain[...]
    blank = jnp.zeros((1, width), F32)
    second = jnp.concatenate([g3[...], g2, blank], axis=1)
    line = lax.broadcasted_iota(jnp.int32, (16, 4 * width), 0)
    gains = jnp.where(line == 0, gm[...], jnp.where(line == 1, second, 0.0)).astype(BF)
    for out in outs:
        xs, rows = out.shape[:2]
        for x in range(xs):
            out[x, rows - 16 :, :] = gains


def tokens_backward(w0, w1, w2, w3, tokens, d_two, gain, sel_back, sel_out, out_o):
    d_normed = pick(sel_back[...], joined((w0, w1, w2, w3)))
    d_norm, _ = norm_back(tokens[...].astype(F32), gain[...], d_normed.astype(F32))
    total = (d_two[...].astype(F32) + d_norm.astype(F32)).astype(BF)
    laid = pick(sel_out[...], total)
    rows, cols = out_o.shape[:2]
    pad = laid.shape[0] // rows
    for r in range(rows):
        out_o[r] = laid[r * pad : r * pad + cols]


def pair_sum(keep, got, *outs):
    for x, out in enumerate(outs):
        out[...] = (keep[x].astype(F32) + got[x].astype(F32)).astype(BF)


def added(parts):
    parts = [p[...].astype(F32) for p in parts]
    while len(parts) > 1:
        half = len(parts) // 2
        parts = [parts[j] + parts[j + half] for j in range(half)]
    return parts[0]


def make_line_sum(rows, near, sub):
    far = rows // near
    size = far * sub

    def line_sum(where, *refs):
        held, outs = refs[: len(refs) - near], refs[len(refs) - near :]
        count = len(held) // 3
        p = lines(rows * sub)
        j, a, k = div(p, size), div(mod(p, size), sub), mod(p, sub)
        row = a * near + mod(mod(where[0], near) + j, near)
        at = 0
        for b in range(3):
            total = added(held[b * count : (b + 1) * count]).astype(BF)
            wanted = row * sub + k
            if b == 2:
                share = total.shape[0] - 16
                part = share // rows
                wanted = jnp.where(k < part, row * part + k, share + k - part)
            laid = pick(one_hot(wanted, total.shape[0]), total)
            for j, out in enumerate(outs):
                out[:, at : at + laid.shape[1]] = laid[j * size : (j + 1) * size]
            at += laid.shape[1]

    def near_sum(where, *refs):
        held, outs = refs[:near], refs[near:]
        total = added(held).astype(BF)
        p = lines(size)
        own = div(where[0], near)
        wanted = mod(own + div(p, sub), far) * sub + mod(p, sub)
        laid = mm(one_hot(wanted, size), total)
        for j, out in enumerate(outs):
            out[...] = laid[j * sub : (j + 1) * sub].astype(BF)

    return line_sum, near_sum


def flat_lines(value, lo, width):
    parts = []
    for r in range(value.shape[0]):
        for at in range(lo, lo + width, TILE):
            parts.append(value[r : r + 1, at : at + TILE])
    return parts


def make_finish(wide, narrow, sub2, far):
    def finish(*refs):
        held, (gains_o, qkv2_o, proj2_o, merge_o, qkv3_o, proj3_o) = refs[:far], refs[far:]
        total = added(held)
        at = 6 * wide
        late = total[:sub2]
        extra = total[sub2 : sub2 + 2]
        first, second = extra[:1], extra[1:]
        gains = (
            flat_lines(second, at + wide, narrow)
            + flat_lines(first, at, 4 * narrow)
            + flat_lines(second, at, wide)
        )
        for out, parts in (
            (gains_o, gains),
            (qkv2_o, flat_lines(late, at, 3 * narrow)),
            (proj2_o, flat_lines(late, at + 3 * narrow, narrow)),
            (merge_o, flat_lines(total, 4 * wide, wide) + flat_lines(total, 5 * wide, wide)),
            (qkv3_o, flat_lines(total, 0, 3 * wide)),
            (proj3_o, flat_lines(total, 3 * wide, wide)),
        ):
            out[...] = jnp.concatenate(parts, axis=0).astype(out.dtype)

    return finish


def call(body, outs, args, flops, scratch=(), scalars=0):
    smem, vmem = (pl.BlockSpec(memory_space=m) for m in (pltpu.SMEM, pltpu.VMEM))
    return pl.pallas_call(
        body,
        in_specs=[smem] * scalars + [vmem] * (len(args) - scalars),
        out_shape=[jax.ShapeDtypeStruct(shape, kind) for shape, kind in outs],
        scratch_shapes=[pltpu.VMEM(shape, kind) for shape, kind in scratch],
        cost_estimate=pl.CostEstimate(flops=flops, transcendentals=0, bytes_accessed=4 << 20),
        compiler_params=pltpu.CompilerParams(vmem_limit_bytes=8 << 20),
    )(*args)


def moved(value, axis, by):
    count = lax.axis_size(axis)
    return lax.ppermute(value, axis, [(i, (i + by) % count) for i in range(count)])


def moved_across(value, by):
    rows, cols = lax.axis_size("rows"), lax.axis_size(COLS)
    pairs = [
        (i * cols + j, ((i + by) % rows) * cols + (j + by) % cols)
        for i in range(rows)
        for j in range(cols)
    ]
    return lax.ppermute(value, ROWS_COLS, pairs)


def to_neighbours(pieces, by):
    rows, cols, corner = pieces
    return moved_across(corner, by), moved(rows, "rows", by), moved(cols, COLS, by)


def exchanged(pieces, by):
    corner, rows, cols = to_neighbours(pieces, by)
    return rows, cols, corner


def core_sum(send, keep):
    got = moved(send, "cols_1", 1)
    shape = (keep.shape[1:], BF)
    return call(pair_sum, [shape] * keep.shape[0], (keep, got), 1 << 26)


def line_parts(blocks):
    return [blocks[0]] + [moved(blocks[j], "cols_0", j) for j in range(1, len(blocks))]


def moved_near(value, by, near):
    count = lax.axis_size("rows")
    pairs = [(i, i - i % near + (i % near + by) % near) for i in range(count)]
    return lax.ppermute(value, "rows", pairs)


def on_device(
    tokens,
    cotangent,
    shift_offsets,
    norm2_gain,
    qkv2,
    proj2,
    merge_gain,
    merge_weight,
    norm3_gain,
    qkv3,
    proj3,
):
    tile_rows, tile_cols, narrow = tokens.shape
    three_rows, three_cols, wide = cotangent.shape
    ranks = tuple(lax.axis_size(a) for a in ROWS_COLS)
    rows, xs, cores = ranks
    pad, pad3 = up16(tile_cols), up16(three_cols)
    size3 = three_rows * pad3
    n2 = (tile_rows // WIN) * (tile_cols // WIN) * SLOT
    n3 = (three_rows // WIN) * (three_cols // WIN) * SLOT
    n4 = 4 * size3
    er, ec, ex = up16(EDGE * tile_cols), up16(tile_rows * EDGE), up16(EDGE * EDGE)
    hr, tr, hc = EDGE * pad3, up16(EDGE * three_cols), up16(three_rows * EDGE)
    gain2, gain_m, gain3 = norm2_gain[None], merge_gain[None], norm3_gain[None]

    edge_sizes = (EDGE * pad, ec, ex)
    parts = wide // narrow
    tokens_p, cot_p, *pieces = call(
        input_edges,
        [
            ((tile_rows * pad, narrow), BF),
            ((size3, wide), BF),
            ((edge_sizes[0] + parts * hr, narrow), BF),
            ((edge_sizes[1] + parts * hc, narrow), BF),
            ((edge_sizes[2] + parts * ex, narrow), BF),
        ],
        (tokens, cotangent),
        1 << 28,
    )
    input_pieces = exchanged(pieces, -1)
    where = jnp.stack([lax.axis_index(a) for a in ROWS_COLS]).astype(jnp.int32)
    early, early_shapes, late, late_shapes = make_tables(
        (tile_rows, tile_cols), (three_rows, three_cols), ranks, (narrow, wide, 4 * narrow)
    )
    scalars = (shift_offsets, where)
    sel_a, tail2, sel_tokens, sel_b, head3, bias2 = call(
        early, early_shapes, scalars, 1 << 28, scalars=2
    )
    sel3, tail3, sel3b, head2, sel_e, sel_out, order2, order3, order_m, bias3 = call(
        late, late_shapes, scalars, 1 << 28, scalars=2
    )

    rolled, packed, mixed, wins, *edges = call(
        functools.partial(two_forward, edge_sizes),
        [
            ((n2, narrow), BF),
            ((n2, 3 * narrow), BF),
            ((n2, narrow), BF),
            ((n2, narrow), BF),
            ((er, narrow), BF),
            ((ec, narrow), BF),
            ((ex, narrow), BF),
        ],
        (tokens_p, *input_pieces, gain2, qkv2, proj2, sel_a, bias2, tail2),
        1 << 30,
    )
    back = exchanged(edges, 1)
    two, tokens_q, merged_norm, merged, normed3, *edges = call(
        merge_forward,
        [
            ((size3, 4 * narrow), BF),
            ((n4, narrow), BF),
            ((size3, 4 * narrow), BF),
            ((size3, wide), BF),
            ((size3, wide), BF),
            ((hr, wide), BF),
            ((hc, wide), BF),
            ((ex, wide), BF),
        ],
        (tokens_p, wins, *back, sel_tokens, sel_b, gain_m, merge_weight, gain3, head3),
        1 << 30,
    )
    ahead = exchanged(edges, -1)
    both, rolled3, above3, mixed3, d_packed3, *edges = call(
        functools.partial(three_both, edge_sizes),
        [
            ((n3, 2 * wide), BF),
            ((n3, wide), BF),
            ((n3, wide), BF),
            ((n3, wide), BF),
            ((n3, 3 * wide), BF),
            ((tr, 2 * wide), BF),
            ((hc, 2 * wide), BF),
            ((ex, 2 * wide), BF),
        ],
        (normed3, *ahead, cot_p, *input_pieces, qkv3, proj3, sel3, bias3, tail3),
        1 << 30,
        scratch=[((n3, 3 * wide), BF), ((n3, wide), BF)],
    )
    back = exchanged(edges, 1)
    share3 = wide // (xs * cores)
    send, keep = call(
        three_grads,
        [((xs, share3, 4 * wide), BF)] * 2,
        (rolled3, above3, mixed3, d_packed3, order3),
        1 << 30,
    )
    sum_a = core_sum(send, keep)
    merged_out, d_two, d_rows, grad_m, grad_3, *edges = call(
        merge_backward,
        [
            ((three_rows, three_cols, wide), BF),
            ((n4, narrow), BF),
            ((size3, wide), BF),
            ((1, 4 * narrow), F32),
            ((1, wide), F32),
            ((er, narrow), BF),
            ((ec, narrow), BF),
            ((ex, narrow), BF),
        ],
        (both, *back, merged, cot_p, two, sel3b, gain3, gain_m, merge_weight, head2),
        1 << 30,
    )
    ahead = exchanged(edges, -1)
    send, keep = call(
        merge_grads, [((xs, share3, 2 * wide), BF)] * 2, (merged_norm, d_rows, order_m), 1 << 30
    )
    sum_b = core_sum(send, keep)
    share2 = narrow // (xs * cores)
    wins, send, keep, *edges = call(
        two_backward,
        [
            ((n2, narrow), BF),
            ((xs, share2 + 16, 4 * narrow), BF),
            ((xs, share2 + 16, 4 * narrow), BF),
            ((er, narrow), BF),
            ((ec, narrow), BF),
            ((ex, narrow), BF),
        ],
        (
            d_two, *ahead, mixed, packed, rolled, qkv2, proj2, gain2, sel_e, bias2, tail2,
            order2, grad_m, grad_3,
        ),
        1 << 30,
        scratch=[((n2, 3 * narrow), BF), ((n2, narrow), BF)],
    )
    back = exchanged(edges, 1)
    sum_c = core_sum(send, keep)
    (tokens_grad,) = call(
        tokens_backward,
        [((tile_rows, tile_cols, narrow), BF)],
        (wins, *back, tokens_q, d_two, gain2, sel_b, sel_out),
        1 << 30,
    )

    sub = wide // (rows * xs * cores)
    sub2 = narrow // (rows * xs * cores)
    far = rows // NEAR
    lanes = 6 * wide + 4 * narrow
    sum_lines, sum_near = make_line_sum(rows, NEAR, sub)
    held = line_parts(sum_a) + line_parts(sum_b) + line_parts(sum_c)
    parts = call(sum_lines, [((far * sub, lanes), BF)] * NEAR, (where, *held), 1 << 26, scalars=1)
    held = [parts[0]] + [moved_near(parts[j], j, NEAR) for j in range(1, NEAR)]
    parts = call(sum_near, [((sub, lanes), BF)] * far, (where, *held), 1 << 26, scalars=1)
    held = [parts[0]] + [moved(parts[j], "rows", j * NEAR) for j in range(1, far)]
    sizes = (
        (narrow + 4 * narrow + wide, F32),
        (sub2 * 3 * narrow, BF),
        (sub2 * narrow, BF),
        (2 * sub * wide, BF),
        (sub * 3 * wide, BF),
        (sub * wide, BF),
    )
    grads = call(
        make_finish(wide, narrow, sub2, far),
        [((size // TILE, TILE), kind) for size, kind in sizes],
        held,
        1 << 26,
    )
    return (merged_out, tokens_grad, *(g.reshape(-1) for g in grads))


def solution(mesh):
    cores = 2
    split = Mesh(
        mesh.devices.reshape(
            mesh.shape["groups"], mesh.shape["rows"], mesh.shape["cols"] // cores, cores
        ),
        ("groups", "rows", "cols_0", "cols_1"),
    )
    tiles = P(("groups", "rows"), COLS, None)
    flat = P(GROUPS_ROWS_COLS)


    return jax.shard_map(
        on_device,
        mesh=split,
        in_specs=(tiles, tiles) + (P(),) * 9,
        out_specs=(tiles, tiles, P("groups"), flat, flat, flat, flat, flat),
        check_vma=False,
    )
```
